256 devices in a mesh: groups: 4 (over x, y), gx: 32 (over z), gy: 2 (over core).
Axes of the slice: x: 2, y: 2, z: 32, core: 2. Of those that a mesh axis runs over, the one named last changes fastest.
The devices are a block of a 4x8x32 slice.
Arguments:
- field: float32 [256, 64, 2048], P(('groups', 'gx'), 'gy'), parts along dimension 0, may hold values from -6 to 6
- spectral: float32 [32, 32, 16, 2, 32, 32], P('gy', 'gx'), may hold values from -2.1213202 to 2.1213202
- conv_first: float32 [3, 3, 3, 32, 32], replicated, may hold values from -0.21875 to 0.21875
- conv_second: float32 [3, 3, 3, 32, 32], replicated, may hold values from -0.21875 to 0.21875
- bias: float32 [32], replicated, may hold values from -3 to 3
Outputs:
- block_output: float32 [256, 64, 2048], P(('groups', 'gx'), 'gy'), parts along dimension 0
The draws below stay inside these ranges and needn't reach their ends.
There are 4 independent parts, one for each index of `groups`. The reference program is written for one: setup_inputs(seed, part) draws one part's arguments, and reference() takes and returns one part's arrays. A program takes and returns all parts, laid end to end along the dimension named above; an argument that names none is the same for every part. Nothing has to cross between parts.
All inputs are finite; a program needn't handle non-finite values.
Results may differ from the reference program's by a relative error of at most 0.000057.
Values sent between devices are 32-bit elements; how exact they have to be, the bound alone decides.
No kernel may reach another device: no remote copies, remote signals or barrier semaphores. Data moves between devices by JAX's collectives and lax.ppermute only.
A program may use at most 128 MiB of HBM per device.

```python
import jax
import jax.numpy as jnp
from jax import lax

CH = 32
NZ = 64
MX = 32
MY = 32
MZ = 16
NX = 64
NY = 64


def shard_levels(stream_key, dims, cuts, smallest, top_value):
    def one(position, parts):
        steps = jax.random.uniform(jax.random.fold_in(jax.random.fold_in(stream_key, 6), position), (parts,), jnp.float32, smallest / len(cuts), top_value / len(cuts))
        return jnp.repeat(jnp.exp(steps), dims[position] // parts).reshape((-1,) + (1,) * (len(dims) - position - 1))

    gain = one(*cuts[0])
    for cut in cuts[1:]:
        gain = gain * one(*cut)
    return gain


def gaussian(stream_key, extent, scale, reach, split=(), kind=jnp.bfloat16):
    drawn = jax.random.normal(stream_key, extent, jnp.float32) * scale
    if len(split) > 0:
        drawn = shard_levels(stream_key, extent, split, -0.22, 0.18) * drawn
    return jnp.clip(drawn, min=-reach, max=reach).astype(kind)


def setup_inputs(seed: int = 0, part: int = 0) -> dict:
    seeds = jax.random.split(jax.random.key(seed), 6)
    part_splits = jax.random.split(jax.random.fold_in(seeds[5], part), 6)
    field = gaussian(part_splits[0], (NX, NY, NZ * CH), 1.0, 6.0, ((0, 32), (1, 2)), jnp.float32)
    spectral = gaussian(seeds[1], (MY, MX, MZ, 2, CH, CH), (2 / CH ** 0.5), 2.1213202, ((0, 2), (1, 32)), jnp.float32)
    conv_first = gaussian(seeds[2], (3, 3, 3, CH, CH), (27 * CH) ** -0.5, 0.21875, (), jnp.float32)
    conv_second = gaussian(seeds[3], (3, 3, 3, CH, CH), (27 * CH) ** -0.5, 0.21875, (), jnp.float32)
    bias = gaussian(seeds[4], (CH,), 0.5, 3.0, (), jnp.float32)
    return dict(field=field, spectral=spectral, conv_first=conv_first, conv_second=conv_second, bias=bias)


def positions(length, retained):
    counter = jnp.arange(retained, dtype=jnp.int32)
    return jnp.where(counter < retained // 2, counter, length - retained + counter)


def convolve(volume, weight):
    return lax.conv_general_dilated(volume[None], weight, (1, 1, 1), "SAME", dimension_numbers=("NDHWC", "DHWIO", "NDHWC"), precision=lax.Precision.HIGHEST)[0]


def reference(field, spectral, conv_first, conv_second, bias):
    volume = field.reshape(NX, NY, NZ, CH)
    spectrum = jnp.fft.rfftn(volume, axes=(0, 1, 2))
    rows_x = positions(NX, MX)
    rows_y = positions(NY, MY)
    retained_modes = spectrum[rows_x][:, rows_y][:, :, :MZ]
    matrix = spectral[:, :, :, 0] + 1j * spectral[:, :, :, 1]
    mixed = jnp.einsum("abzi,bazio->abzo", retained_modes, matrix, precision=lax.Precision.HIGHEST)
    full_spectrum = jnp.zeros(spectrum.shape, spectrum.dtype).at[rows_x[:, None], rows_y[None, :], :MZ].set(mixed)
    spectral_part = jnp.fft.irfftn(full_spectrum, s=(NX, NY, NZ), axes=(0, 1, 2))
    first_hidden = jax.nn.gelu(convolve(volume, conv_first), approximate=False)
    second_branch = convolve(first_hidden, conv_second)
    result = jax.nn.gelu(spectral_part + second_branch + bias, approximate=False)
    return result.reshape(NX, NY, NZ * CH)
```

```python
import functools
import math

import jax
import jax.numpy as jnp
import numpy as np
from jax import lax
from jax.experimental import pallas as pl
from jax.experimental.pallas import tpu as pltpu
from jax.sharding import PartitionSpec as P

CH = 32
NZ = 64
MX = 32
MY = 32
MZ = 16

LANES = 128
GROUP = LANES // CH
ZQ = NZ // GROUP
ROWS = 8
F32 = jnp.float32
BF16 = jnp.bfloat16
VMEM = pl.BlockSpec(memory_space=pltpu.VMEM)


def small_grant():
    return pltpu.CompilerParams(vmem_limit_bytes=12 << 20)


def split(value):
    high = value.astype(BF16)
    return high, (value - high.astype(F32)).astype(BF16)


def host_split(table):
    table = np.asarray(table, np.float32)
    high = table.astype(jnp.bfloat16)
    low = (table - high.astype(np.float32)).astype(jnp.bfloat16)
    return np.stack([high, low])


def dot(a, b):
    return jnp.dot(a, b, preferred_element_type=F32)


def dot3(table_high, table_low, value):
    high, low = split(value)
    return dot(table_high, high) + (dot(table_low, high) + dot(table_high, low))


def gelu(v):
    return v * (1.0 + lax.erf(v * (1.0 / math.sqrt(2.0)))) * 0.5


def kept(count, length):
    return np.array([j if j < count // 2 else length - count + j for j in range(count)])


def rotation(angle):
    return np.array([[np.cos(angle), -np.sin(angle)], [np.sin(angle), np.cos(angle)]])


def forward_tables(cells_x, cells_y, devices_y):
    extent = cells_y * devices_y
    freq = kept(MY, extent)
    owned = MY // devices_y
    table = np.zeros((devices_y, devices_y, owned, cells_x, 2, 2, cells_x, cells_y))
    for g in range(devices_y):
        places = g * cells_y + np.arange(cells_y)
        for t in range(devices_y):
            rows = freq[t * owned : (t + 1) * owned]
            turn = rotation(-2 * np.pi * (rows[:, None] * places[None, :] % extent) / extent)
            for x in range(cells_x):
                table[g, t, :, x, :, :, x, :] = turn.transpose(2, 0, 1, 3)
    return table.reshape(devices_y, devices_y, owned * cells_x * 2, 2 * cells_x * cells_y)


def z_twiddle(sign):
    zr = np.repeat(np.arange(GROUP), CH)
    angle = sign * 2 * np.pi * np.arange(MZ)[:, None] * zr[None, :] / NZ
    return np.stack([np.cos(angle), np.sin(angle)]).astype(np.float32)


def z_forward(blocks, twiddle, lane):
    half = ZQ // 2
    even = [None] + [blocks[n] + blocks[ZQ - n] for n in range(1, half)]
    odd = [None] + [blocks[n] - blocks[ZQ - n] for n in range(1, half)]
    real, imag = [], []
    for k in range(half + 1):
        re = blocks[0] + blocks[half] if k % 2 == 0 else blocks[0] - blocks[half]
        im = None
        for n in range(1, half):
            c = math.cos(2 * math.pi * (k * n % ZQ) / ZQ)
            s = math.sin(2 * math.pi * (k * n % ZQ) / ZQ)
            if abs(c) > 1e-9:
                re = re + even[n] * c
            if abs(s) > 1e-9:
                im = odd[n] * -s if im is None else im - odd[n] * s
        real.append(re)
        imag.append(im)
    out = ([], [])
    upper = lane >= LANES // 2
    odd_group = (lane // CH) % 2 == 1
    for first in range(0, MZ, GROUP):
        pieces = ([], [])
        for k in range(first, first + GROUP):
            fold = k if k <= half else ZQ - k
            fr, fi = real[fold], imag[fold]
            if fi is not None and k > half:
                fi = -fi
            tc, ts = twiddle(k)
            if fi is None:
                pieces[0].append(fr * tc)
                pieces[1].append(fr * ts)
            else:
                pieces[0].append(fr * tc - fi * ts)
                pieces[1].append(fi * tc + fr * ts)
        for part in range(2):
            y0, y1, y2, y3 = pieces[part]
            a = jnp.where(upper, y2, y0) + pltpu.roll(jnp.where(upper, y0, y2), LANES // 2, 1)
            b = jnp.where(upper, y3, y1) + pltpu.roll(jnp.where(upper, y1, y3), LANES // 2, 1)
            out[part].append(
                jnp.where(odd_group, b + pltpu.roll(b, CH, 1), a + pltpu.roll(a, LANES - CH, 1))
            )
    return out


def forward_kernel(cells_ref, table_ref, twiddle_ref, keep_ref, send_ref, z_ref, *, devices_y):
    rows = cells_ref.shape[0]
    lane = lax.broadcasted_iota(jnp.int32, (ROWS, LANES), 1)

    def step(i, carry):
        start = pl.multiple_of(i * ROWS, ROWS)
        blocks = [cells_ref[pl.ds(start, ROWS), q * LANES : (q + 1) * LANES] for q in range(ZQ)]

        def twiddle(k):
            return (
                jnp.broadcast_to(twiddle_ref[0, k : k + 1, :], (ROWS, LANES)),
                jnp.broadcast_to(twiddle_ref[1, k : k + 1, :], (ROWS, LANES)),
            )

        real, imag = z_forward(blocks, twiddle, lane)
        for h in range(MZ // GROUP):
            z_ref[pl.ds(start, ROWS), h * LANES : (h + 1) * LANES] = real[h]
            z_ref[pl.ds(start + rows, ROWS), h * LANES : (h + 1) * LANES] = imag[h]
        return carry

    lax.fori_loop(0, rows // ROWS, step, 0)
    here = lax.axis_index("gy")
    there = devices_y - 1 - here
    high, low = split(z_ref[...])
    for target, out_ref in ((there, send_ref), (here, keep_ref)):
        table = table_ref[here, target, 0]
        modes = dot(table, high) + (dot(table_ref[here, target, 1], high) + dot(table, low))
        for h in range(MZ // GROUP):
            for kp in range(modes.shape[0] // ROWS):
                out_ref[kp * (MZ // GROUP) + h] = modes[
                    kp * ROWS : (kp + 1) * ROWS, h * LANES : (h + 1) * LANES
                ]


def x_tables(cells_x, devices_x, pair):
    extent = cells_x * devices_x
    freq = kept(MX, extent)
    place = np.arange(extent)
    forward = np.zeros((MX, pair, 2, devices_x, pair, cells_x, 2))
    inverse = np.zeros((devices_x, pair, cells_x, 2, MX, pair, 2))
    angle = 2 * np.pi * (freq[:, None] * place[None, :] % extent) / extent
    turn = rotation(-angle).reshape(2, 2, MX, devices_x, cells_x)
    back = rotation(angle).reshape(2, 2, MX, devices_x, cells_x)
    for q in range(pair):
        forward[:, q, :, :, q] = turn.transpose(2, 0, 3, 4, 1)
        inverse[:, q, :, :, :, q] = back.transpose(3, 4, 0, 2, 1)
    return (
        forward.reshape(MX * pair * 2, devices_x * pair * cells_x * 2),
        inverse.reshape(devices_x * pair * cells_x * 2, MX * pair * 2),
    )


def matrix_kernel(table_ref, value_ref, out_ref):
    out_ref[...] = dot3(table_ref[0], table_ref[1], value_ref[...])


def apply_matrix(table, value):
    return pl.pallas_call(
        matrix_kernel,
        out_shape=jax.ShapeDtypeStruct((table.shape[1], value.shape[1]), F32),
        in_specs=[VMEM, VMEM],
        out_specs=VMEM,
        compiler_params=small_grant(),
    )(table, value)


def mix_kernel(modes_ref, weight_ref, out_ref):
    count = modes_ref.shape[0] // 2
    halves = GROUP * count // LANES
    per = GROUP // halves
    parts = []
    for part in range(2):
        turned = modes_ref[pl.ds(part, count, stride=2), :].T
        parts.append(
            [
                jnp.concatenate(
                    [turned[(h * per + g) * CH : (h * per + g + 1) * CH] for g in range(per)],
                    axis=1,
                )
                for h in range(halves)
            ]
        )
    outs = ([], [])
    for h in range(halves):
        re, im = parts[0][h], parts[1][h]
        acc_re = jnp.zeros((CH, LANES), F32)
        acc_im = jnp.zeros((CH, LANES), F32)
        for c in range(CH):
            wr = weight_ref[0, h, c]
            wi = weight_ref[1, h, c]
            a = re[c : c + 1, :]
            b = im[c : c + 1, :]
            acc_re = acc_re + (a * wr - b * wi)
            acc_im = acc_im + (a * wi + b * wr)
        for g in range(per):
            outs[0].append(acc_re[:, g * count : (g + 1) * count])
            outs[1].append(acc_im[:, g * count : (g + 1) * count])
    for part in range(2):
        out_ref[pl.ds(part, count, stride=2), :] = jnp.concatenate(outs[part], axis=0).T


def inverse_tables(cells_x, cells_y, devices_y):
    extent = cells_y * devices_y
    freq = kept(MY, extent)
    owned = MY // devices_y
    table = np.zeros((devices_y, devices_y, 2, cells_x, cells_y, owned, cells_x, 2))
    for g in range(devices_y):
        places = g * cells_y + np.arange(cells_y)
        for t in range(devices_y):
            rows = freq[t * owned : (t + 1) * owned]
            turn = rotation(2 * np.pi * (places[:, None] * rows[None, :] % extent) / extent)
            for x in range(cells_x):
                table[g, t, :, x, :, :, x, :] = turn.transpose(0, 2, 3, 1)
    return table.reshape(devices_y, devices_y, 2 * cells_x * cells_y, owned * cells_x * 2)


def end_kernel(
    own_ref, other_ref, table_ref, twiddle_ref, branch_ref, bias_ref, out_ref, y_ref, *, devices_y
):
    here = lax.axis_index("gy")
    there = devices_y - 1 - here
    wide = MZ // GROUP
    rows = out_ref.shape[0]

    def gather(ref):
        pairs = ref.shape[0] // wide
        return jnp.concatenate(
            [
                jnp.concatenate([ref[kp * wide + h] for kp in range(pairs)], axis=0)
                for h in range(wide)
            ],
            axis=1,
        )

    y_ref[...] = dot3(table_ref[here, here, 0], table_ref[here, here, 1], gather(own_ref)) + dot3(
        table_ref[here, there, 0], table_ref[here, there, 1], gather(other_ref)
    )
    lane = lax.broadcasted_iota(jnp.int32, (ROWS, LANES), 1)
    group = lane // CH
    half = ZQ // 2

    def step(i, carry):
        start = pl.multiple_of(i * ROWS, ROWS)

        def spread(value, g):
            kept_lanes = jnp.where(group == g, value, 0.0)
            kept_lanes = kept_lanes + pltpu.roll(kept_lanes, LANES // 2, 1)
            return kept_lanes + pltpu.roll(kept_lanes, CH, 1)

        real, imag = [], []
        for k in range(MZ):
            h, g = divmod(k, GROUP)
            re = spread(y_ref[pl.ds(start, ROWS), h * LANES : (h + 1) * LANES], g)
            im = spread(y_ref[pl.ds(start + rows, ROWS), h * LANES : (h + 1) * LANES], g)
            tc = jnp.broadcast_to(twiddle_ref[0, k : k + 1, :], (ROWS, LANES))
            ts = jnp.broadcast_to(twiddle_ref[1, k : k + 1, :], (ROWS, LANES))
            real.append(re * tc - im * ts)
            imag.append(re * ts + im * tc)
        even = [None] + [real[k] + real[ZQ - k] for k in range(1, half)]
        odd = [None] + [imag[k] - imag[ZQ - k] for k in range(1, half)]
        bias = jnp.broadcast_to(bias_ref[...], (ROWS, LANES))
        for q in range(half + 1):
            cos_part = real[0] + real[half] if q % 2 == 0 else real[0] - real[half]
            cos_part = cos_part + bias
            sin_part = None
            for k in range(1, half):
                c = math.cos(2 * math.pi * (k * q % ZQ) / ZQ)
                s = math.sin(2 * math.pi * (k * q % ZQ) / ZQ)
                if abs(c) > 1e-9:
                    cos_part = cos_part + even[k] * c
                if abs(s) > 1e-9:
                    sin_part = odd[k] * s if sin_part is None else sin_part + odd[k] * s
            places = [(q, -1.0)] if sin_part is None else [(q, -1.0), (ZQ - q, 1.0)]
            for place, sign in places:
                value = cos_part
                if sin_part is not None:
                    value = cos_part + sin_part if sign > 0 else cos_part - sin_part
                lanes = slice(place * LANES, (place + 1) * LANES)
                value = value + branch_ref[pl.ds(start, ROWS), lanes]
                out_ref[pl.ds(start, ROWS), lanes] = gelu(value)
        return carry

    lax.fori_loop(0, rows // ROWS, step, 0)


BLOCK = 8
WINDOW = BLOCK + 2 * GROUP
TOP = 8


def conv_kernel(
    cells_ref, before_ref, after_ref, rim_ref, weight_ref, out_ref, pad_ref, high_ref, low_ref,
    table_high_ref, table_low_ref, acc_ref, *, activate,
):
    cells_x, cells_y, width = cells_ref.shape
    here = lax.axis_index("gy")
    blocks = NZ // BLOCK
    out_lanes = BLOCK * CH
    in_lanes = WINDOW * CH

    lane = lax.broadcasted_iota(jnp.int32, (CH, out_lanes), 1)
    group = lane // CH
    repeat = jnp.where(
        lax.broadcasted_iota(jnp.int32, (CH, out_lanes), 0) == lane % CH, 1.0, 0.0
    ).astype(BF16)
    zero = jnp.zeros((CH, out_lanes), BF16)

    def build(i, carry):
        for value, ref in zip(split(weight_ref[i]), (table_high_ref, table_low_ref), strict=True):
            wide = dot(value, repeat)
            for z in range(WINDOW):
                total = None
                for e in range(3):
                    place = z - (GROUP - 1) - e
                    if 0 <= place < BLOCK:
                        term = jnp.where(group == place, wide[e * CH : (e + 1) * CH], 0.0)
                        total = term if total is None else total + term
                ref[i, z * CH : (z + 1) * CH, :] = zero if total is None else total.astype(BF16)
        return carry

    lax.fori_loop(0, 9, build, 0)

    pad_ref[:, :, :LANES] = jnp.zeros((cells_x + 2, pad_ref.shape[1], LANES), F32)
    pad_ref[:, :, LANES + width :] = jnp.zeros((cells_x + 2, pad_ref.shape[1], LANES), F32)
    inner = slice(LANES, LANES + width)
    pad_ref[0, TOP : TOP + cells_y, inner] = before_ref[0]
    for x in range(cells_x):
        pad_ref[1 + x, TOP : TOP + cells_y, inner] = cells_ref[x]
    pad_ref[1 + cells_x, TOP : TOP + cells_y, inner] = after_ref[0]
    for x in range(cells_x + 2):
        row = rim_ref[x : x + 1, :]
        pad_ref[x, TOP - 1 : TOP, inner] = jnp.where(here == 0, 0.0, row)
        pad_ref[x, TOP + cells_y : TOP + cells_y + 1, inner] = jnp.where(here == 0, row, 0.0)

    def fill(x, carry):
        for shift in range(3):
            for z in range(blocks):
                value = pad_ref[
                    x,
                    TOP - 1 + shift : TOP - 1 + shift + cells_y,
                    z * out_lanes : z * out_lanes + in_lanes,
                ]
                high, low = split(value)
                high_ref[shift, z, x] = high
                low_ref[shift, z, x] = low
        return carry

    lax.fori_loop(0, cells_x + 2, fill, 0)

    acc_ref[...] = jnp.zeros(acc_ref.shape, F32)

    def multiply(i, carry):
        shift_x = i // 3
        shift_y = i % 3
        rows = blocks * cells_x * cells_y
        high = high_ref[shift_y, :, pl.ds(shift_x, cells_x)].reshape(rows, in_lanes)
        low = low_ref[shift_y, :, pl.ds(shift_x, cells_x)].reshape(rows, in_lanes)
        table_high = table_high_ref[i]
        acc_ref[...] += dot(high, table_high) + (
            dot(high, table_low_ref[i]) + dot(low, table_high)
        )
        return carry

    lax.fori_loop(0, 9, multiply, 0)
    for z in range(blocks):
        for x in range(cells_x):
            start = (z * cells_x + x) * cells_y
            value = acc_ref[start : start + cells_y, :]
            out_ref[x, :, z * out_lanes : (z + 1) * out_lanes] = gelu(value) if activate else value


def convolve(cells, weight, activate):
    cells_x, cells_y, width = cells.shape
    count = lax.axis_size("gx")
    before = lax.ppermute(cells[cells_x - 1 :], "gx", [(i, i + 1) for i in range(count - 1)])
    after = lax.ppermute(cells[:1], "gx", [(i + 1, i) for i in range(count - 1)])
    planes = (before, cells, after)
    first = jnp.concatenate([plane[:, 0] for plane in planes], axis=0)
    last = jnp.concatenate([plane[:, cells_y - 1] for plane in planes], axis=0)
    rim = lax.ppermute(
        jnp.where(lax.axis_index("gy") == 0, last, first), "gy", [(0, 1), (1, 0)]
    )
    blocks = NZ // BLOCK
    rows = blocks * cells_x * cells_y
    return pl.pallas_call(
        functools.partial(conv_kernel, activate=activate),
        out_shape=jax.ShapeDtypeStruct(cells.shape, F32),
        in_specs=[VMEM] * 5,
        out_specs=VMEM,
        scratch_shapes=[
            pltpu.VMEM((cells_x + 2, cells_y + 2 * TOP, width + 2 * LANES), F32),
            pltpu.VMEM((3, blocks, cells_x + 2, cells_y, WINDOW * CH), BF16),
            pltpu.VMEM((3, blocks, cells_x + 2, cells_y, WINDOW * CH), BF16),
            pltpu.VMEM((9, WINDOW * CH, BLOCK * CH), BF16),
            pltpu.VMEM((9, WINDOW * CH, BLOCK * CH), BF16),
            pltpu.VMEM((rows, BLOCK * CH), F32),
        ],
        compiler_params=pltpu.CompilerParams(vmem_limit_bytes=22 << 20),
        cost_estimate=pl.CostEstimate(
            flops=6 * rows * 9 * WINDOW * CH * BLOCK * CH, transcendentals=0, bytes_accessed=1 << 21
        ),
    )(cells, before, after, rim, weight.reshape(9, 3 * CH, CH))


def all_to_all(value):
    return lax.all_to_all(value, "gx", split_axis=0, concat_axis=0, tiled=True)


def block(field, spectral, conv_first, conv_second, bias):
    cells_x, cells_y, width = field.shape
    devices_x = lax.axis_size("gx")
    devices_y = lax.axis_size("gy")
    extent_x = cells_x * devices_x
    extent_y = cells_y * devices_y
    owned_y = MY // devices_y
    wide = MZ // GROUP
    pair = ROWS // (2 * cells_x)
    tiles = owned_y // pair * wide
    assert devices_y == 2 and tiles == devices_x and MX == devices_x

    forward_y = np.moveaxis(host_split(forward_tables(cells_x, cells_y, devices_y)), 0, 2)
    inverse_y = np.moveaxis(host_split(inverse_tables(cells_x, cells_y, devices_y)), 0, 2)
    forward_x, inverse_x = (host_split(t) for t in x_tables(cells_x, devices_x, pair))
    twiddle_out = z_twiddle(1)
    weights = np.where(np.arange(MZ) == 0, 1.0, 2.0) / (extent_x * extent_y * NZ)
    twiddle_out = (twiddle_out * weights[None, :, None]).astype(np.float32)

    tile_shape = jax.ShapeDtypeStruct((tiles, ROWS, LANES), F32)
    keep, send = pl.pallas_call(
        functools.partial(forward_kernel, devices_y=devices_y),
        out_shape=(tile_shape, tile_shape),
        in_specs=[VMEM] * 3,
        out_specs=(VMEM, VMEM),
        scratch_shapes=[pltpu.VMEM((2 * cells_x * cells_y, MZ * CH), F32)],
        compiler_params=small_grant(),
    )(field.reshape(cells_x * cells_y, width), forward_y, z_twiddle(-1))
    lines = keep + lax.ppermute(send, "gy", [(0, 1), (1, 0)])
    lines, cells, spectral = lax.optimization_barrier((lines, field, spectral))

    columns = all_to_all(lines)
    hidden = convolve(cells, conv_first, True)
    modes = apply_matrix(forward_x, columns.reshape(-1, LANES))
    modes = all_to_all(modes.reshape(MX, 2 * pair, LANES))

    count = tiles * pair
    halves = GROUP * count // LANES
    matrix = spectral.reshape(
        owned_y // pair, pair, wide, halves, GROUP // halves, 2, CH, CH
    ).transpose(5, 3, 6, 7, 4, 0, 2, 1)
    matrix = matrix.reshape(2, halves, CH, CH, LANES)
    mixed = pl.pallas_call(
        mix_kernel,
        out_shape=jax.ShapeDtypeStruct((2 * count, LANES), F32),
        in_specs=[VMEM, VMEM],
        out_specs=VMEM,
        compiler_params=small_grant(),
    )(modes.reshape(2 * count, LANES), matrix)
    columns = all_to_all(mixed.reshape(tiles, 2 * pair, LANES))
    branch = convolve(hidden, conv_second, False)
    lines = apply_matrix(inverse_x, columns.reshape(-1, LANES))
    own = all_to_all(lines.reshape(devices_x, ROWS, LANES))
    other = lax.ppermute(own, "gy", [(0, 1), (1, 0)])
    result = pl.pallas_call(
        functools.partial(end_kernel, devices_y=devices_y),
        out_shape=jax.ShapeDtypeStruct((cells_x * cells_y, width), F32),
        in_specs=[VMEM] * 6,
        out_specs=VMEM,
        scratch_shapes=[pltpu.VMEM((2 * cells_x * cells_y, MZ * CH), F32)],
        compiler_params=small_grant(),
    )(
        own, other, inverse_y, twiddle_out, branch.reshape(cells_x * cells_y, width),
        jnp.tile(bias, GROUP).reshape(1, LANES),
    )
    return result.reshape(cells_x, cells_y, width)


def solution(mesh):
    in_specs = (
        P(("groups", "gx"), "gy", None),
        P("gy", "gx", None, None, None, None),
        P(),
        P(),
        P(),
    )
    out_specs = P(("groups", "gx"), "gy", None)
    return jax.shard_map(block, mesh=mesh, in_specs=in_specs, out_specs=out_specs, check_vma=False)
```

```python
import functools
import math

import jax
import jax.numpy as jnp
import numpy as np
from jax import lax
from jax.experimental import pallas as pl
from jax.experimental.pallas import tpu as pltpu
from jax.sharding import PartitionSpec as P

CH = 32
NZ = 64
MX = 32
MY = 32
MZ = 16

LANES = 128
GROUP = LANES // CH
ZQ = NZ // GROUP
ROWS = 8
F32 = jnp.float32
BF16 = jnp.bfloat16
VMEM = pl.BlockSpec(memory_space=pltpu.VMEM)


def small_grant():
    return pltpu.CompilerParams(vmem_limit_bytes=12 << 20)


def split(value):
    high = value.astype(BF16)
    return high, (value - high.astype(F32)).astype(BF16)


def host_split(table):
    table = np.asarray(table, np.float32)
    high = table.astype(jnp.bfloat16)
    low = (table - high.astype(np.float32)).astype(jnp.bfloat16)
    return np.stack([high, low])


def dot(a, b):
    return jnp.dot(a, b, preferred_element_type=F32)


def dot3(table_high, table_low, value):
    high, low = split(value)
    return dot(table_high, high) + (dot(table_low, high) + dot(table_high, low))


def gelu(v):
    return v * (1.0 + lax.erf(v * (1.0 / math.sqrt(2.0)))) * 0.5


def kept(count, length):
    return np.array([j if j < count // 2 else length - count + j for j in range(count)])


def rotation(angle):
    return np.array([[np.cos(angle), -np.sin(angle)], [np.sin(angle), np.cos(angle)]])


def forward_tables(cells_x, cells_y, devices_y):
    extent = cells_y * devices_y
    freq = kept(MY, extent)
    owned = MY // devices_y
    table = np.zeros((devices_y, devices_y, owned, cells_x, 2, 2, cells_x, cells_y))
    for g in range(devices_y):
        places = g * cells_y + np.arange(cells_y)
        for t in range(devices_y):
            rows = freq[t * owned : (t + 1) * owned]
            turn = rotation(-2 * np.pi * (rows[:, None] * places[None, :] % extent) / extent)
            for x in range(cells_x):
                table[g, t, :, x, :, :, x, :] = turn.transpose(2, 0, 1, 3)
    return table.reshape(devices_y, devices_y, owned * cells_x * 2, 2 * cells_x * cells_y)


def z_twiddle(sign):
    zr = np.repeat(np.arange(GROUP), CH)
    angle = sign * 2 * np.pi * np.arange(MZ)[:, None] * zr[None, :] / NZ
    return np.stack([np.cos(angle), np.sin(angle)]).astype(np.float32)


def z_forward(blocks, twiddle, lane):
    half = ZQ // 2
    even = [None] + [blocks[n] + blocks[ZQ - n] for n in range(1, half)]
    odd = [None] + [blocks[n] - blocks[ZQ - n] for n in range(1, half)]
    real, imag = [], []
    for k in range(half + 1):
        re = blocks[0] + blocks[half] if k % 2 == 0 else blocks[0] - blocks[half]
        im = None
        for n in range(1, half):
            c = math.cos(2 * math.pi * (k * n % ZQ) / ZQ)
            s = math.sin(2 * math.pi * (k * n % ZQ) / ZQ)
            if abs(c) > 1e-9:
                re = re + even[n] * c
            if abs(s) > 1e-9:
                im = odd[n] * -s if im is None else im - odd[n] * s
        real.append(re)
        imag.append(im)
    out = ([], [])
    upper = lane >= LANES // 2
    odd_group = (lane // CH) % 2 == 1
    for first in range(0, MZ, GROUP):
        pieces = ([], [])
        for k in range(first, first + GROUP):
            fold = k if k <= half else ZQ - k
            fr, fi = real[fold], imag[fold]
            if fi is not None and k > half:
                fi = -fi
            tc, ts = twiddle(k)
            if fi is None:
                pieces[0].append(fr * tc)
                pieces[1].append(fr * ts)
            else:
                pieces[0].append(fr * tc - fi * ts)
                pieces[1].append(fi * tc + fr * ts)
        for part in range(2):
            y0, y1, y2, y3 = pieces[part]
            a = jnp.where(upper, y2, y0) + pltpu.roll(jnp.where(upper, y0, y2), LANES // 2, 1)
            b = jnp.where(upper, y3, y1) + pltpu.roll(jnp.where(upper, y1, y3), LANES // 2, 1)
            out[part].append(
                jnp.where(odd_group, b + pltpu.roll(b, CH, 1), a + pltpu.roll(a, LANES - CH, 1))
            )
    return out


def forward_kernel(
    cells_hbm, table_hbm, twiddle_hbm, keep_ref, send_ref, z_ref, cells_ref, table_ref,
    twiddle_ref, sems, *, devices_y,
):
    rows = cells_ref.shape[0]
    here = lax.axis_index("gy")
    there = devices_y - 1 - here
    lane = lax.broadcasted_iota(jnp.int32, (ROWS, LANES), 1)
    half_rows = rows // 2
    twiddle_copy = pltpu.make_async_copy(twiddle_hbm, twiddle_ref, sems.at[0])
    table_copy = pltpu.make_async_copy(table_hbm.at[here], table_ref, sems.at[1])
    cell_copies = [
        pltpu.make_async_copy(
            cells_hbm.at[pl.ds(part * half_rows, half_rows)],
            cells_ref.at[pl.ds(part * half_rows, half_rows)],
            sems.at[2 + part],
        )
        for part in range(2)
    ]
    twiddle_copy.start()
    cell_copies[0].start()
    cell_copies[1].start()
    table_copy.start()
    twiddle_copy.wait()

    def step(i, carry):
        start = pl.multiple_of(i * ROWS, ROWS)
        blocks = [cells_ref[pl.ds(start, ROWS), q * LANES : (q + 1) * LANES] for q in range(ZQ)]

        def twiddle(k):
            return (
                jnp.broadcast_to(twiddle_ref[0, k : k + 1, :], (ROWS, LANES)),
                jnp.broadcast_to(twiddle_ref[1, k : k + 1, :], (ROWS, LANES)),
            )

        real, imag = z_forward(blocks, twiddle, lane)
        for h in range(MZ // GROUP):
            z_ref[pl.ds(start, ROWS), h * LANES : (h + 1) * LANES] = real[h]
            z_ref[pl.ds(start + rows, ROWS), h * LANES : (h + 1) * LANES] = imag[h]
        return carry

    steps = half_rows // ROWS
    for part in range(2):
        cell_copies[part].wait()
        lax.fori_loop(part * steps, (part + 1) * steps, step, 0)
    table_copy.wait()
    high, low = split(z_ref[...])
    for target, out_ref in ((there, send_ref), (here, keep_ref)):
        table = table_ref[target, 0]
        modes = dot(table, high) + (dot(table_ref[target, 1], high) + dot(table, low))
        for h in range(MZ // GROUP):
            for kp in range(modes.shape[0] // ROWS):
                out_ref[h * (modes.shape[0] // ROWS) + kp] = modes[
                    kp * ROWS : (kp + 1) * ROWS, h * LANES : (h + 1) * LANES
                ]


def x_tables(cells_x, devices_x, pair):
    extent = cells_x * devices_x
    freq = kept(MX, extent)
    place = np.arange(extent)
    forward = np.zeros((MX, pair, 2, devices_x, pair, cells_x, 2))
    inverse = np.zeros((devices_x, pair, cells_x, 2, MX, pair, 2))
    angle = 2 * np.pi * (freq[:, None] * place[None, :] % extent) / extent
    turn = rotation(-angle).reshape(2, 2, MX, devices_x, cells_x)
    back = rotation(angle).reshape(2, 2, MX, devices_x, cells_x)
    for q in range(pair):
        forward[:, q, :, :, q] = turn.transpose(2, 0, 3, 4, 1)
        inverse[:, q, :, :, :, q] = back.transpose(3, 4, 0, 2, 1)
    return (
        forward.reshape(MX * pair * 2, devices_x * pair * cells_x * 2),
        inverse.reshape(devices_x * pair * cells_x * 2, MX * pair * 2),
    )


def matrix_kernel(table_ref, value_ref, out_ref):
    out_ref[...] = dot3(table_ref[0], table_ref[1], value_ref[...])


def apply_matrix(table, value):
    return pl.pallas_call(
        matrix_kernel,
        out_shape=jax.ShapeDtypeStruct((table.shape[1], value.shape[1]), F32),
        in_specs=[VMEM, VMEM],
        out_specs=VMEM,
        compiler_params=small_grant(),
    )(table, value)


def arrange_kernel(weight_ref, out_ref, *, owned_y):
    halves, channels = out_ref.shape[1:3]
    wide = MZ // GROUP
    per = GROUP // halves
    stride = MZ * 2 * channels

    def step(c, carry):
        for part in range(2):
            for h in range(halves):
                pieces = []
                for g in range(per):
                    for block in range(wide):
                        kz = block * GROUP + h * per + g
                        first = (kz * 2 + part) * channels + c
                        pieces.append(weight_ref[pl.ds(first, owned_y, stride=stride), :])
                out_ref[part, h, c] = jnp.concatenate(pieces, axis=0).T
        return carry

    lax.fori_loop(0, channels, step, 0)


def mix_kernel(modes_ref, weight_ref, out_ref):
    count = modes_ref.shape[0] // 2
    halves = GROUP * count // LANES
    per = GROUP // halves
    parts = []
    for part in range(2):
        turned = modes_ref[pl.ds(part, count, stride=2), :].T
        parts.append(
            [
                jnp.concatenate(
                    [turned[(h * per + g) * CH : (h * per + g + 1) * CH] for g in range(per)],
                    axis=1,
                )
                for h in range(halves)
            ]
        )
    outs = ([], [])
    for h in range(halves):
        re, im = parts[0][h], parts[1][h]
        acc_re = jnp.zeros((CH, LANES), F32)
        acc_im = jnp.zeros((CH, LANES), F32)
        for c in range(CH):
            wr = weight_ref[0, h, c]
            wi = weight_ref[1, h, c]
            a = re[c : c + 1, :]
            b = im[c : c + 1, :]
            acc_re = acc_re + (a * wr - b * wi)
            acc_im = acc_im + (a * wi + b * wr)
        for g in range(per):
            outs[0].append(acc_re[:, g * count : (g + 1) * count])
            outs[1].append(acc_im[:, g * count : (g + 1) * count])
    for part in range(2):
        out_ref[pl.ds(part, count, stride=2), :] = jnp.concatenate(outs[part], axis=0).T


def inverse_tables(cells_x, cells_y, devices_y):
    extent = cells_y * devices_y
    freq = kept(MY, extent)
    owned = MY // devices_y
    table = np.zeros((devices_y, devices_y, 2, cells_x, cells_y, owned, cells_x, 2))
    for g in range(devices_y):
        places = g * cells_y + np.arange(cells_y)
        for t in range(devices_y):
            rows = freq[t * owned : (t + 1) * owned]
            turn = rotation(2 * np.pi * (places[:, None] * rows[None, :] % extent) / extent)
            for x in range(cells_x):
                table[g, t, :, x, :, :, x, :] = turn.transpose(0, 2, 3, 1)
    return table.reshape(devices_y, devices_y, 2 * cells_x * cells_y, owned * cells_x * 2)


def end_kernel(
    own_ref, other_ref, table_ref, twiddle_ref, branch_ref, bias_ref, out_ref, y_ref, *, devices_y
):
    here = lax.axis_index("gy")
    there = devices_y - 1 - here
    wide = MZ // GROUP
    rows = out_ref.shape[0]

    def gather(ref):
        pairs = ref.shape[0] // wide
        return jnp.concatenate(
            [
                jnp.concatenate([ref[h * pairs + kp] for kp in range(pairs)], axis=0)
                for h in range(wide)
            ],
            axis=1,
        )

    y_ref[...] = dot3(table_ref[here, here, 0], table_ref[here, here, 1], gather(own_ref)) + dot3(
        table_ref[here, there, 0], table_ref[here, there, 1], gather(other_ref)
    )
    lane = lax.broadcasted_iota(jnp.int32, (ROWS, LANES), 1)
    group = lane // CH
    half = ZQ // 2

    def step(i, carry):
        start = pl.multiple_of(i * ROWS, ROWS)

        def spread(value, g):
            kept_lanes = jnp.where(group == g, value, 0.0)
            kept_lanes = kept_lanes + pltpu.roll(kept_lanes, LANES // 2, 1)
            return kept_lanes + pltpu.roll(kept_lanes, CH, 1)

        real, imag = [], []
        for k in range(MZ):
            h, g = divmod(k, GROUP)
            re = spread(y_ref[pl.ds(start, ROWS), h * LANES : (h + 1) * LANES], g)
            im = spread(y_ref[pl.ds(start + rows, ROWS), h * LANES : (h + 1) * LANES], g)
            tc = jnp.broadcast_to(twiddle_ref[0, k : k + 1, :], (ROWS, LANES))
            ts = jnp.broadcast_to(twiddle_ref[1, k : k + 1, :], (ROWS, LANES))
            real.append(re * tc - im * ts)
            imag.append(re * ts + im * tc)
        even = [None] + [real[k] + real[ZQ - k] for k in range(1, half)]
        odd = [None] + [imag[k] - imag[ZQ - k] for k in range(1, half)]
        bias = jnp.broadcast_to(bias_ref[...], (ROWS, LANES))
        for q in range(half + 1):
            cos_part = real[0] + real[half] if q % 2 == 0 else real[0] - real[half]
            cos_part = cos_part + bias
            sin_part = None
            for k in range(1, half):
                c = math.cos(2 * math.pi * (k * q % ZQ) / ZQ)
                s = math.sin(2 * math.pi * (k * q % ZQ) / ZQ)
                if abs(c) > 1e-9:
                    cos_part = cos_part + even[k] * c
                if abs(s) > 1e-9:
                    sin_part = odd[k] * s if sin_part is None else sin_part + odd[k] * s
            places = [(q, -1.0)] if sin_part is None else [(q, -1.0), (ZQ - q, 1.0)]
            for place, sign in places:
                value = cos_part
                if sin_part is not None:
                    value = cos_part + sin_part if sign > 0 else cos_part - sin_part
                lanes = slice(place * LANES, (place + 1) * LANES)
                value = value + branch_ref[pl.ds(start, ROWS), lanes]
                out_ref[pl.ds(start, ROWS), lanes] = gelu(value)
        return carry

    lax.fori_loop(0, rows // ROWS, step, 0)


BLOCK = 8
WINDOW = BLOCK + 2 * GROUP
TOP = 8


def conv_kernel(
    first_ref, second_ref, rim_ref, weight_ref, out_ref, pad_ref, high_ref, low_ref,
    table_high_ref, table_low_ref, acc_ref, *, shifted, activate,
):
    cells_ref = first_ref
    cells_x, cells_y, width = cells_ref.shape
    here = lax.axis_index("gy")
    blocks = NZ // BLOCK
    out_lanes = BLOCK * CH
    in_lanes = WINDOW * CH

    lane = lax.broadcasted_iota(jnp.int32, (CH, out_lanes), 1)
    group = lane // CH
    repeat = jnp.where(
        lax.broadcasted_iota(jnp.int32, (CH, out_lanes), 0) == lane % CH, 1.0, 0.0
    ).astype(BF16)
    zero = jnp.zeros((CH, out_lanes), BF16)

    def build(i, carry):
        for value, ref in zip(split(weight_ref[i]), (table_high_ref, table_low_ref), strict=True):
            wide = dot(value, repeat)
            for z in range(WINDOW):
                total = None
                for e in range(3):
                    place = z - (GROUP - 1) - e
                    if 0 <= place < BLOCK:
                        other = 0.0 if total is None else total
                        total = jnp.where(group == place, wide[e * CH : (e + 1) * CH], other)
                ref[i, z * CH : (z + 1) * CH, :] = zero if total is None else total.astype(BF16)
        return carry

    lax.fori_loop(0, 9, build, 0)

    pad_ref[:, :, :LANES] = jnp.zeros((2 * cells_x, pad_ref.shape[1], LANES), F32)
    pad_ref[:, :, LANES + width :] = jnp.zeros((2 * cells_x, pad_ref.shape[1], LANES), F32)
    inner = slice(LANES, LANES + width)
    for x in range(cells_x):
        pad_ref[x, TOP : TOP + cells_y, inner] = first_ref[x]
        pad_ref[cells_x + x, TOP : TOP + cells_y, inner] = second_ref[x]
    for x in range(2 * cells_x):
        row = rim_ref[x : x + 1, :]
        pad_ref[x, TOP - 1 : TOP, inner] = jnp.where(here == 0, 0.0, row)
        pad_ref[x, TOP + cells_y : TOP + cells_y + 1, inner] = jnp.where(here == 0, row, 0.0)

    place = lax.axis_index("gx")
    at_start = place == 0
    at_end = place == lax.axis_size("gx") - 1

    def fill(slot, carry):
        x = (slot + 1) // 2
        if shifted:
            outside = at_end & ((slot == 1) | (slot == 4))
        else:
            outside = (at_start & (slot == 0)) | (at_end & (slot == 5))
        inside = jnp.where(outside, 0.0, 1.0)
        for shift in range(3):
            for z in range(blocks):
                value = pad_ref[
                    x,
                    TOP - 1 + shift : TOP - 1 + shift + cells_y,
                    z * out_lanes : z * out_lanes + in_lanes,
                ]
                high, low = split(value * inside)
                high_ref[shift, z, slot] = high
                low_ref[shift, z, slot] = low
        return carry

    lax.fori_loop(0, 3 * cells_x, fill, 0)

    acc_ref[...] = jnp.zeros(acc_ref.shape, F32)

    def multiply(i, carry):
        shift_x = i // 3
        shift_y = i % 3
        rows = blocks * cells_x * cells_y
        high = high_ref[shift_y, :, pl.ds(shift_x * cells_x, cells_x)].reshape(rows, in_lanes)
        low = low_ref[shift_y, :, pl.ds(shift_x * cells_x, cells_x)].reshape(rows, in_lanes)
        table_high = table_high_ref[i]
        acc_ref[...] += dot(high, table_high) + (
            dot(high, table_low_ref[i]) + dot(low, table_high)
        )
        return carry

    lax.fori_loop(0, 9, multiply, 0)
    for z in range(blocks):
        for x in range(cells_x):
            start = (z * cells_x + x) * cells_y
            value = acc_ref[start : start + cells_y, :]
            out_ref[x, :, z * out_lanes : (z + 1) * out_lanes] = gelu(value) if activate else value


def rim_kernel(first_top, first_end, second_top, second_end, out_ref):
    here = lax.axis_index("gy")
    for i, (top, end) in enumerate(((first_top, first_end), (second_top, second_end))):
        for x in range(top.shape[0]):
            row = jnp.where(here == 0, end[x, ROWS - 1 : ROWS, :], top[x, 0:1, :])
            out_ref[i * top.shape[0] + x : i * top.shape[0] + x + 1, :] = row


def convolve(first, second, weight, shifted, activate):
    cells_x, cells_y, width = first.shape
    top = pl.BlockSpec((cells_x, ROWS, width), lambda i: (0, 0, 0))
    end = pl.BlockSpec((cells_x, ROWS, width), lambda i: (0, cells_y // ROWS - 1, 0))
    rim = pl.pallas_call(
        rim_kernel,
        grid=(1,),
        out_shape=jax.ShapeDtypeStruct((2 * cells_x, width), F32),
        in_specs=[top, end, top, end],
        out_specs=pl.BlockSpec((2 * cells_x, width), lambda i: (0, 0)),
        compiler_params=small_grant(),
    )(first, first, second, second)
    rim = lax.ppermute(rim, "gy", [(0, 1), (1, 0)])
    return band_product(first, second, rim, weight, shifted, activate)


def band_product(first, second, rim, weight, shifted, activate):
    cells_x, cells_y, width = first.shape
    blocks = NZ // BLOCK
    rows = blocks * cells_x * cells_y
    return pl.pallas_call(
        functools.partial(conv_kernel, shifted=shifted, activate=activate),
        out_shape=jax.ShapeDtypeStruct(first.shape, F32),
        in_specs=[VMEM] * 4,
        out_specs=VMEM,
        scratch_shapes=[
            pltpu.VMEM((2 * cells_x, cells_y + 2 * TOP, width + 2 * LANES), F32),
            pltpu.VMEM((3, blocks, 3 * cells_x, cells_y, WINDOW * CH), BF16),
            pltpu.VMEM((3, blocks, 3 * cells_x, cells_y, WINDOW * CH), BF16),
            pltpu.VMEM((9, WINDOW * CH, BLOCK * CH), BF16),
            pltpu.VMEM((9, WINDOW * CH, BLOCK * CH), BF16),
            pltpu.VMEM((rows, BLOCK * CH), F32),
        ],
        compiler_params=pltpu.CompilerParams(vmem_limit_bytes=20 << 20),
        cost_estimate=pl.CostEstimate(
            flops=6 * rows * 9 * WINDOW * CH * BLOCK * CH, transcendentals=0, bytes_accessed=1 << 21
        ),
    )(first, second, rim, weight.reshape(9, 3 * CH, CH))


def all_to_all(value):
    return lax.all_to_all(value, "gx", split_axis=0, concat_axis=0, tiled=True)


def block(field, spectral, conv_first, conv_second, bias):
    cells_x, cells_y, width = field.shape
    devices_x = lax.axis_size("gx")
    devices_y = lax.axis_size("gy")
    extent_x = cells_x * devices_x
    extent_y = cells_y * devices_y
    owned_y = MY // devices_y
    wide = MZ // GROUP
    pair = ROWS // (2 * cells_x)
    tiles = owned_y // pair * wide
    assert devices_y == 2 and cells_x == 2 and tiles == devices_x and MX == devices_x

    forward_y = np.moveaxis(host_split(forward_tables(cells_x, cells_y, devices_y)), 0, 2)
    inverse_y = np.moveaxis(host_split(inverse_tables(cells_x, cells_y, devices_y)), 0, 2)
    forward_x, inverse_x = (host_split(t) for t in x_tables(cells_x, devices_x, pair))
    twiddle_out = z_twiddle(1)
    weights = np.where(np.arange(MZ) == 0, 1.0, 2.0) / (extent_x * extent_y * NZ)
    twiddle_out = (twiddle_out * weights[None, :, None]).astype(np.float32)

    tile_shape = jax.ShapeDtypeStruct((tiles, ROWS, LANES), F32)
    keep, send = pl.pallas_call(
        functools.partial(forward_kernel, devices_y=devices_y),
        out_shape=(tile_shape, tile_shape),
        in_specs=[pl.BlockSpec(memory_space=pltpu.HBM)] * 3,
        out_specs=(VMEM, VMEM),
        scratch_shapes=[
            pltpu.VMEM((2 * cells_x * cells_y, MZ * CH), F32),
            pltpu.VMEM((cells_x * cells_y, width), F32),
            pltpu.VMEM(forward_y.shape[1:], BF16),
            pltpu.VMEM((2, MZ, LANES), F32),
            pltpu.SemaphoreType.DMA((4,)),
        ],
        compiler_params=pltpu.CompilerParams(vmem_limit_bytes=58 << 20),
    )(field.reshape(cells_x * cells_y, width), forward_y, z_twiddle(-1))
    lines = keep + lax.ppermute(send, "gy", [(0, 1), (1, 0)])
    lines, cells, spectral = lax.optimization_barrier((lines, field, spectral))

    columns = all_to_all(lines)
    following = lax.ppermute(
        cells, "gx", [((i + 1) % devices_x, i) for i in range(devices_x)]
    )
    hidden = convolve(cells, following, conv_first, True, True)
    modes = apply_matrix(forward_x, columns.reshape(-1, LANES))
    modes = all_to_all(modes.reshape(MX, 2 * pair, LANES))

    count = tiles * pair
    halves = GROUP * count // LANES
    matrix = pl.pallas_call(
        functools.partial(arrange_kernel, owned_y=owned_y),
        out_shape=jax.ShapeDtypeStruct((2, halves, CH, CH, LANES), F32),
        in_specs=[VMEM],
        out_specs=VMEM,
        compiler_params=pltpu.CompilerParams(vmem_limit_bytes=24 << 20),
        cost_estimate=pl.CostEstimate(flops=1 << 30, transcendentals=0, bytes_accessed=10 << 20),
    )(spectral.reshape(-1, CH))
    mixed = pl.pallas_call(
        mix_kernel,
        out_shape=jax.ShapeDtypeStruct((2 * count, LANES), F32),
        in_specs=[VMEM, VMEM],
        out_specs=VMEM,
        compiler_params=small_grant(),
    )(modes.reshape(2 * count, LANES), matrix)
    columns = all_to_all(mixed.reshape(tiles, 2 * pair, LANES))
    previous = lax.ppermute(
        hidden, "gx", [(i, (i + 1) % devices_x) for i in range(devices_x)]
    )
    branch = convolve(previous, hidden, conv_second, False, False)
    lines = apply_matrix(inverse_x, columns.reshape(-1, LANES))
    own = all_to_all(lines.reshape(devices_x, ROWS, LANES))
    other = lax.ppermute(own, "gy", [(0, 1), (1, 0)])
    result = pl.pallas_call(
        functools.partial(end_kernel, devices_y=devices_y),
        out_shape=jax.ShapeDtypeStruct((cells_x * cells_y, width), F32),
        in_specs=[VMEM] * 6,
        out_specs=VMEM,
        scratch_shapes=[pltpu.VMEM((2 * cells_x * cells_y, MZ * CH), F32)],
        compiler_params=small_grant(),
    )(
        own, other, inverse_y, twiddle_out, branch.reshape(cells_x * cells_y, width),
        jnp.tile(bias, GROUP).reshape(1, LANES),
    )
    return result.reshape(cells_x, cells_y, width)


def solution(mesh):
    in_specs = (
        P(("groups", "gx"), "gy", None),
        P("gy", "gx", None, None, None, None),
        P(),
        P(),
        P(),
    )
    out_specs = P(("groups", "gx"), "gy", None)
    return jax.shard_map(block, mesh=mesh, in_specs=in_specs, out_specs=out_specs, check_vma=False)
```

```python
import functools
import math

import jax
import jax.numpy as jnp
import numpy as np
from jax import lax
from jax.experimental import pallas as pl
from jax.experimental.pallas import tpu as pltpu
from jax.sharding import PartitionSpec as P

CH = 32
NZ = 64
MX = 32
MY = 32
MZ = 16

LANES = 128
GROUP = LANES // CH
ZQ = NZ // GROUP
ROWS = 8
F32 = jnp.float32
BF16 = jnp.bfloat16
VMEM = pl.BlockSpec(memory_space=pltpu.VMEM)


def small_grant():
    return pltpu.CompilerParams(vmem_limit_bytes=12 << 20)


def split(value):
    high = value.astype(BF16)
    return high, (value - high.astype(F32)).astype(BF16)


def host_split(table):
    table = np.asarray(table, np.float32)
    high = table.astype(jnp.bfloat16)
    low = (table - high.astype(np.float32)).astype(jnp.bfloat16)
    return np.stack([high, low])


def dot(a, b):
    return jnp.dot(a, b, preferred_element_type=F32)


def dot3(table_high, table_low, value):
    high, low = split(value)
    return dot(table_high, high) + (dot(table_low, high) + dot(table_high, low))


def gelu(v):
    return v * (1.0 + lax.erf(v * (1.0 / math.sqrt(2.0)))) * 0.5


def kept(count, length):
    return np.array([j if j < count // 2 else length - count + j for j in range(count)])


def rotation(angle):
    return np.array([[np.cos(angle), -np.sin(angle)], [np.sin(angle), np.cos(angle)]])


def forward_tables(cells_x, cells_y, devices_y):
    extent = cells_y * devices_y
    freq = kept(MY, extent)
    owned = MY // devices_y
    table = np.zeros((devices_y, devices_y, owned, cells_x, 2, 2, cells_x, cells_y))
    for g in range(devices_y):
        places = g * cells_y + np.arange(cells_y)
        for t in range(devices_y):
            rows = freq[t * owned : (t + 1) * owned]
            turn = rotation(-2 * np.pi * (rows[:, None] * places[None, :] % extent) / extent)
            for x in range(cells_x):
                table[g, t, :, x, :, :, x, :] = turn.transpose(2, 0, 1, 3)
    return table.reshape(devices_y, devices_y, owned * cells_x * 2, 2 * cells_x * cells_y)


def z_twiddle(sign):
    zr = np.repeat(np.arange(GROUP), CH)
    angle = sign * 2 * np.pi * np.arange(MZ)[:, None] * zr[None, :] / NZ
    return np.stack([np.cos(angle), np.sin(angle)]).astype(np.float32)


def z_forward(blocks, twiddle, lane):
    half = ZQ // 2
    even = [None] + [blocks[n] + blocks[ZQ - n] for n in range(1, half)]
    odd = [None] + [blocks[n] - blocks[ZQ - n] for n in range(1, half)]
    real, imag = [], []
    for k in range(half + 1):
        re = blocks[0] + blocks[half] if k % 2 == 0 else blocks[0] - blocks[half]
        im = None
        for n in range(1, half):
            c = math.cos(2 * math.pi * (k * n % ZQ) / ZQ)
            s = math.sin(2 * math.pi * (k * n % ZQ) / ZQ)
            if abs(c) > 1e-9:
                re = re + even[n] * c
            if abs(s) > 1e-9:
                im = odd[n] * -s if im is None else im - odd[n] * s
        real.append(re)
        imag.append(im)
    out = ([], [])
    upper = lane >= LANES // 2
    odd_group = (lane // CH) % 2 == 1
    for first in range(0, MZ, GROUP):
        pieces = ([], [])
        for k in range(first, first + GROUP):
            fold = k if k <= half else ZQ - k
            fr, fi = real[fold], imag[fold]
            if fi is not None and k > half:
                fi = -fi
            tc, ts = twiddle(k)
            if fi is None:
                pieces[0].append(fr * tc)
                pieces[1].append(fr * ts)
            else:
                pieces[0].append(fr * tc - fi * ts)
                pieces[1].append(fi * tc + fr * ts)
        for part in range(2):
            y0, y1, y2, y3 = pieces[part]
            a = jnp.where(upper, y2, y0) + pltpu.roll(jnp.where(upper, y0, y2), LANES // 2, 1)
            b = jnp.where(upper, y3, y1) + pltpu.roll(jnp.where(upper, y1, y3), LANES // 2, 1)
            out[part].append(
                jnp.where(odd_group, b + pltpu.roll(b, CH, 1), a + pltpu.roll(a, LANES - CH, 1))
            )
    return out


def forward_kernel(cells_ref, table_ref, keep_ref, send_ref, z_ref, *, devices_y):
    rows = cells_ref.shape[0]
    here = lax.axis_index("gy")
    there = devices_y - 1 - here
    size = keep_ref.shape[0] * ROWS // (MZ // GROUP)
    twiddles = devices_y * devices_y * size
    lane = lax.broadcasted_iota(jnp.int32, (ROWS, LANES), 1)

    def step(i, carry):
        start = pl.multiple_of(i * ROWS, ROWS)
        blocks = [cells_ref[pl.ds(start, ROWS), q * LANES : (q + 1) * LANES] for q in range(ZQ)]

        def twiddle(k):
            return tuple(
                jnp.broadcast_to(table_ref[row : row + 1, :], (ROWS, LANES))
                for row in (twiddles + k, twiddles + MZ + k)
            )

        real, imag = z_forward(blocks, twiddle, lane)
        for h in range(MZ // GROUP):
            z_ref[pl.ds(start, ROWS), h * LANES : (h + 1) * LANES] = real[h]
            z_ref[pl.ds(start + rows, ROWS), h * LANES : (h + 1) * LANES] = imag[h]
        return carry

    lax.fori_loop(0, rows // ROWS, step, 0)
    high, low = split(z_ref[...])
    for target, out_ref in ((there, send_ref), (here, keep_ref)):
        first = pl.multiple_of((here * devices_y + target) * size, size)
        table, table_low = split(table_ref[pl.ds(first, size), :])
        modes = dot(table, high) + (dot(table_low, high) + dot(table, low))
        for h in range(MZ // GROUP):
            for kp in range(modes.shape[0] // ROWS):
                out_ref[h * (modes.shape[0] // ROWS) + kp] = modes[
                    kp * ROWS : (kp + 1) * ROWS, h * LANES : (h + 1) * LANES
                ]


def x_tables(cells_x, devices_x, pair):
    extent = cells_x * devices_x
    freq = kept(MX, extent)
    place = np.arange(extent)
    forward = np.zeros((MX, pair, 2, devices_x, pair, cells_x, 2))
    inverse = np.zeros((devices_x, pair, cells_x, 2, MX, pair, 2))
    angle = 2 * np.pi * (freq[:, None] * place[None, :] % extent) / extent
    turn = rotation(-angle).reshape(2, 2, MX, devices_x, cells_x)
    back = rotation(angle).reshape(2, 2, MX, devices_x, cells_x)
    for q in range(pair):
        forward[:, q, :, :, q] = turn.transpose(2, 0, 3, 4, 1)
        inverse[:, q, :, :, :, q] = back.transpose(3, 4, 0, 2, 1)
    return (
        forward.reshape(MX * pair * 2, devices_x * pair * cells_x * 2),
        inverse.reshape(devices_x * pair * cells_x * 2, MX * pair * 2),
    )


def matrix_kernel(table_ref, value_ref, out_ref):
    out_ref[...] = dot3(table_ref[0], table_ref[1], value_ref[...])


def apply_matrix(table, value):
    return pl.pallas_call(
        matrix_kernel,
        out_shape=jax.ShapeDtypeStruct((table.shape[1], value.shape[1]), F32),
        in_specs=[VMEM, VMEM],
        out_specs=VMEM,
        compiler_params=small_grant(),
    )(table, value)


def prepare_kernel(weight_ref, high_ref, low_ref):
    depth = high_ref.shape[2]

    def step(i, carry):
        for block in range(MZ // GROUP):
            first = block * GROUP * depth
            value = jnp.concatenate(
                [
                    weight_ref[i, first + g * depth : first + (g + 1) * depth, :]
                    for g in range(GROUP)
                ],
                axis=1,
            )
            high_ref[block, i], low_ref[block, i] = split(value)
        return carry

    lax.fori_loop(0, weight_ref.shape[0], step, 0)


def mix_kernel(modes_ref, weight_high_ref, weight_low_ref, out_ref):
    owned_y, depth = weight_high_ref.shape[1:3]
    channels = depth // 2
    span = owned_y * depth
    repeats = span // LANES
    lane = lax.broadcasted_iota(jnp.int32, (owned_y, LANES), 1)
    group = lane // channels
    second = group % 2 == 1
    both_group = lax.broadcasted_iota(jnp.int32, (2 * owned_y, LANES), 1) // channels
    wide_lane = lax.broadcasted_iota(jnp.int32, (2 * owned_y, span), 1)
    wide_row = lax.broadcasted_iota(jnp.int32, (2 * owned_y, span), 0)
    own = wide_lane // depth == wide_row % owned_y

    def spread(value, g):
        value = jnp.where(group == g, value, 0.0)
        value = value + pltpu.roll(value, LANES // 2, 1)
        return value + pltpu.roll(value, channels, 1)

    for block in range(MZ // GROUP):
        first = block * 2 * owned_y
        real = modes_ref[pl.ds(first, owned_y, stride=2), :]
        imag = modes_ref[pl.ds(first + 1, owned_y, stride=2), :]
        left = ([], [])
        for g in range(GROUP):
            re, im = spread(real, g), spread(imag, g)
            pair = jnp.concatenate([jnp.where(second, -im, re), jnp.where(second, re, im)], axis=0)
            for part, value in zip(left, split(pair), strict=True):
                wide = jnp.concatenate([value.astype(F32)] * repeats, axis=1)
                part.append(jnp.where(own, wide, 0.0).astype(BF16))
        high, low = (jnp.concatenate(part, axis=0) for part in left)
        weight_high = weight_high_ref[block].reshape(span, LANES)
        weight_low = weight_low_ref[block].reshape(span, LANES)
        total = dot(high, weight_high) + (dot(low, weight_high) + dot(high, weight_low))
        mixed = total[: 2 * owned_y]
        for g in range(1, GROUP):
            mixed = jnp.where(
                both_group == g, total[g * 2 * owned_y : (g + 1) * 2 * owned_y], mixed
            )
        out_ref[pl.ds(first, owned_y, stride=2), :] = mixed[:owned_y]
        out_ref[pl.ds(first + 1, owned_y, stride=2), :] = mixed[owned_y:]


def inverse_tables(cells_x, cells_y, devices_y):
    extent = cells_y * devices_y
    freq = kept(MY, extent)
    owned = MY // devices_y
    table = np.zeros((devices_y, devices_y, 2, cells_x, cells_y, owned, cells_x, 2))
    for g in range(devices_y):
        places = g * cells_y + np.arange(cells_y)
        for t in range(devices_y):
            rows = freq[t * owned : (t + 1) * owned]
            turn = rotation(2 * np.pi * (places[:, None] * rows[None, :] % extent) / extent)
            for x in range(cells_x):
                table[g, t, :, x, :, :, x, :] = turn.transpose(0, 2, 3, 1)
    return table.reshape(devices_y, devices_y, 2 * cells_x * cells_y, owned * cells_x * 2)


def end_kernel(
    own_ref, other_ref, table_ref, twiddle_ref, branch_ref, bias_ref, out_ref, y_ref, *, devices_y
):
    here = lax.axis_index("gy")
    there = devices_y - 1 - here
    wide = MZ // GROUP
    rows = out_ref.shape[0]

    def gather(ref):
        pairs = ref.shape[0] // wide
        return jnp.concatenate(
            [
                jnp.concatenate([ref[h * pairs + kp] for kp in range(pairs)], axis=0)
                for h in range(wide)
            ],
            axis=1,
        )

    y_ref[...] = dot3(table_ref[here, here, 0], table_ref[here, here, 1], gather(own_ref)) + dot3(
        table_ref[here, there, 0], table_ref[here, there, 1], gather(other_ref)
    )
    lane = lax.broadcasted_iota(jnp.int32, (ROWS, LANES), 1)
    group = lane // CH
    half = ZQ // 2

    def step(i, carry):
        start = pl.multiple_of(i * ROWS, ROWS)

        def spread(value, g):
            kept_lanes = jnp.where(group == g, value, 0.0)
            kept_lanes = kept_lanes + pltpu.roll(kept_lanes, LANES // 2, 1)
            return kept_lanes + pltpu.roll(kept_lanes, CH, 1)

        real, imag = [], []
        for k in range(MZ):
            h, g = divmod(k, GROUP)
            re = spread(y_ref[pl.ds(start, ROWS), h * LANES : (h + 1) * LANES], g)
            im = spread(y_ref[pl.ds(start + rows, ROWS), h * LANES : (h + 1) * LANES], g)
            tc = jnp.broadcast_to(twiddle_ref[0, k : k + 1, :], (ROWS, LANES))
            ts = jnp.broadcast_to(twiddle_ref[1, k : k + 1, :], (ROWS, LANES))
            real.append(re * tc - im * ts)
            imag.append(re * ts + im * tc)
        even = [None] + [real[k] + real[ZQ - k] for k in range(1, half)]
        odd = [None] + [imag[k] - imag[ZQ - k] for k in range(1, half)]
        bias = jnp.broadcast_to(bias_ref[...], (ROWS, LANES))
        for q in range(half + 1):
            cos_part = real[0] + real[half] if q % 2 == 0 else real[0] - real[half]
            cos_part = cos_part + bias
            sin_part = None
            for k in range(1, half):
                c = math.cos(2 * math.pi * (k * q % ZQ) / ZQ)
                s = math.sin(2 * math.pi * (k * q % ZQ) / ZQ)
                if abs(c) > 1e-9:
                    cos_part = cos_part + even[k] * c
                if abs(s) > 1e-9:
                    sin_part = odd[k] * s if sin_part is None else sin_part + odd[k] * s
            places = [(q, -1.0)] if sin_part is None else [(q, -1.0), (ZQ - q, 1.0)]
            for place, sign in places:
                value = cos_part
                if sin_part is not None:
                    value = cos_part + sin_part if sign > 0 else cos_part - sin_part
                lanes = slice(place * LANES, (place + 1) * LANES)
                value = value + branch_ref[pl.ds(start, ROWS), lanes]
                out_ref[pl.ds(start, ROWS), lanes] = gelu(value)
        return carry

    lax.fori_loop(0, rows // ROWS, step, 0)


BLOCK = 8
WINDOW = BLOCK + 2 * GROUP
TOP = 8


def conv_kernel(
    first_ref, second_ref, rim_ref, weight_ref, out_ref, pad_ref, high_ref, low_ref,
    table_high_ref, table_low_ref, acc_ref, *, shifted, activate,
):
    cells_ref = first_ref
    cells_x, cells_y, width = cells_ref.shape
    here = lax.axis_index("gy")
    blocks = NZ // BLOCK
    out_lanes = BLOCK * CH
    in_lanes = WINDOW * CH

    lane = lax.broadcasted_iota(jnp.int32, (CH, out_lanes), 1)
    group = lane // CH
    repeat = jnp.where(
        lax.broadcasted_iota(jnp.int32, (CH, out_lanes), 0) == lane % CH, 1.0, 0.0
    ).astype(BF16)
    zero = jnp.zeros((CH, out_lanes), BF16)

    def build(i, carry):
        for value, ref in zip(split(weight_ref[i]), (table_high_ref, table_low_ref), strict=True):
            wide = dot(value, repeat)
            for z in range(WINDOW):
                total = None
                for e in range(3):
                    place = z - (GROUP - 1) - e
                    if 0 <= place < BLOCK:
                        other = 0.0 if total is None else total
                        total = jnp.where(group == place, wide[e * CH : (e + 1) * CH], other)
                ref[i, z * CH : (z + 1) * CH, :] = zero if total is None else total.astype(BF16)
        return carry

    lax.fori_loop(0, 9, build, 0)

    pad_ref[:, :, :LANES] = jnp.zeros((2 * cells_x, pad_ref.shape[1], LANES), F32)
    pad_ref[:, :, LANES + width :] = jnp.zeros((2 * cells_x, pad_ref.shape[1], LANES), F32)
    inner = slice(LANES, LANES + width)
    for x in range(cells_x):
        pad_ref[x, TOP : TOP + cells_y, inner] = first_ref[x]
        pad_ref[cells_x + x, TOP : TOP + cells_y, inner] = second_ref[x]
    for x in range(2 * cells_x):
        row = rim_ref[x : x + 1, :]
        pad_ref[x, TOP - 1 : TOP, inner] = jnp.where(here == 0, 0.0, row)
        pad_ref[x, TOP + cells_y : TOP + cells_y + 1, inner] = jnp.where(here == 0, row, 0.0)

    place = lax.axis_index("gx")
    at_start = place == 0
    at_end = place == lax.axis_size("gx") - 1

    def fill(slot, carry):
        x = (slot + 1) // 2
        if shifted:
            outside = at_end & ((slot == 1) | (slot == 4))
        else:
            outside = (at_start & (slot == 0)) | (at_end & (slot == 5))
        inside = jnp.where(outside, 0.0, 1.0)
        for shift in range(3):
            for z in range(blocks):
                value = pad_ref[
                    x,
                    TOP - 1 + shift : TOP - 1 + shift + cells_y,
                    z * out_lanes : z * out_lanes + in_lanes,
                ]
                high, low = split(value * inside)
                high_ref[shift, z, slot] = high
                low_ref[shift, z, slot] = low
        return carry

    lax.fori_loop(0, 3 * cells_x, fill, 0)

    acc_ref[...] = jnp.zeros(acc_ref.shape, F32)

    def multiply(i, carry):
        shift_x = i // 3
        shift_y = i % 3
        rows = blocks * cells_x * cells_y
        high = high_ref[shift_y, :, pl.ds(shift_x * cells_x, cells_x)].reshape(rows, in_lanes)
        low = low_ref[shift_y, :, pl.ds(shift_x * cells_x, cells_x)].reshape(rows, in_lanes)
        table_high = table_high_ref[i]
        acc_ref[...] += dot(high, table_high) + (
            dot(high, table_low_ref[i]) + dot(low, table_high)
        )
        return carry

    lax.fori_loop(0, 9, multiply, 0)
    for z in range(blocks):
        for x in range(cells_x):
            start = (z * cells_x + x) * cells_y
            value = acc_ref[start : start + cells_y, :]
            out_ref[x, :, z * out_lanes : (z + 1) * out_lanes] = gelu(value) if activate else value


def rim_kernel(first_top, first_end, second_top, second_end, out_ref):
    here = lax.axis_index("gy")
    for i, (top, end) in enumerate(((first_top, first_end), (second_top, second_end))):
        for x in range(top.shape[0]):
            row = jnp.where(here == 0, end[x, ROWS - 1 : ROWS, :], top[x, 0:1, :])
            out_ref[i * top.shape[0] + x : i * top.shape[0] + x + 1, :] = row


def convolve(first, second, weight, shifted, activate):
    cells_x, cells_y, width = first.shape
    top = pl.BlockSpec((cells_x, ROWS, width), lambda i: (0, 0, 0))
    end = pl.BlockSpec((cells_x, ROWS, width), lambda i: (0, cells_y // ROWS - 1, 0))
    rim = pl.pallas_call(
        rim_kernel,
        grid=(1,),
        out_shape=jax.ShapeDtypeStruct((2 * cells_x, width), F32),
        in_specs=[top, end, top, end],
        out_specs=pl.BlockSpec((2 * cells_x, width), lambda i: (0, 0)),
        compiler_params=small_grant(),
    )(first, first, second, second)
    rim = lax.ppermute(rim, "gy", [(0, 1), (1, 0)])
    return band_product(first, second, rim, weight, shifted, activate)


def band_product(first, second, rim, weight, shifted, activate):
    cells_x, cells_y, width = first.shape
    blocks = NZ // BLOCK
    rows = blocks * cells_x * cells_y
    return pl.pallas_call(
        functools.partial(conv_kernel, shifted=shifted, activate=activate),
        out_shape=jax.ShapeDtypeStruct(first.shape, F32),
        in_specs=[VMEM] * 4,
        out_specs=VMEM,
        scratch_shapes=[
            pltpu.VMEM((2 * cells_x, cells_y + 2 * TOP, width + 2 * LANES), F32),
            pltpu.VMEM((3, blocks, 3 * cells_x, cells_y, WINDOW * CH), BF16),
            pltpu.VMEM((3, blocks, 3 * cells_x, cells_y, WINDOW * CH), BF16),
            pltpu.VMEM((9, WINDOW * CH, BLOCK * CH), BF16),
            pltpu.VMEM((9, WINDOW * CH, BLOCK * CH), BF16),
            pltpu.VMEM((rows, BLOCK * CH), F32),
        ],
        compiler_params=pltpu.CompilerParams(vmem_limit_bytes=20 << 20),
        cost_estimate=pl.CostEstimate(
            flops=6 * rows * 9 * WINDOW * CH * BLOCK * CH, transcendentals=0, bytes_accessed=1 << 21
        ),
    )(first, second, rim, weight.reshape(9, 3 * CH, CH))


def all_to_all(value):
    return lax.all_to_all(value, "gx", split_axis=0, concat_axis=0, tiled=True)


def block(field, spectral, conv_first, conv_second, bias):
    cells_x, cells_y, width = field.shape
    devices_x = lax.axis_size("gx")
    devices_y = lax.axis_size("gy")
    extent_x = cells_x * devices_x
    extent_y = cells_y * devices_y
    owned_y = MY // devices_y
    wide = MZ // GROUP
    pair = ROWS // (2 * cells_x)
    tiles = owned_y // pair * wide
    assert devices_y == 2 and cells_x == 2 and tiles == devices_x and MX == devices_x

    forward_y = np.concatenate(
        [
            forward_tables(cells_x, cells_y, devices_y).reshape(-1, 2 * cells_x * cells_y),
            z_twiddle(-1).reshape(-1, LANES),
        ]
    ).astype(np.float32)
    inverse_y = np.moveaxis(host_split(inverse_tables(cells_x, cells_y, devices_y)), 0, 2)
    forward_x, inverse_x = (host_split(t) for t in x_tables(cells_x, devices_x, pair))
    twiddle_out = z_twiddle(1)
    weights = np.where(np.arange(MZ) == 0, 1.0, 2.0) / (extent_x * extent_y * NZ)
    twiddle_out = (twiddle_out * weights[None, :, None]).astype(np.float32)

    tile_shape = jax.ShapeDtypeStruct((tiles, ROWS, LANES), F32)
    keep, send = pl.pallas_call(
        functools.partial(forward_kernel, devices_y=devices_y),
        out_shape=(tile_shape, tile_shape),
        in_specs=[VMEM] * 2,
        out_specs=(VMEM, VMEM),
        scratch_shapes=[pltpu.VMEM((2 * cells_x * cells_y, MZ * CH), F32)],
        compiler_params=small_grant(),
    )(field.reshape(cells_x * cells_y, width), forward_y)
    lines = keep + lax.ppermute(send, "gy", [(0, 1), (1, 0)])
    lines, cells = lax.optimization_barrier((lines, field))

    columns = all_to_all(lines)
    following = lax.ppermute(
        cells, "gx", [((i + 1) % devices_x, i) for i in range(devices_x)]
    )
    hidden = convolve(cells, following, conv_first, True, True)
    modes = apply_matrix(forward_x, columns.reshape(-1, LANES))
    modes = all_to_all(modes.reshape(MX, 2 * pair, LANES))

    count = tiles * pair
    matrix_shape = (wide, owned_y, 2 * CH, LANES)
    matrix = pl.pallas_call(
        prepare_kernel,
        out_shape=(jax.ShapeDtypeStruct(matrix_shape, BF16),) * 2,
        in_specs=[VMEM],
        out_specs=(VMEM, VMEM),
        compiler_params=pltpu.CompilerParams(vmem_limit_bytes=20 << 20),
        cost_estimate=pl.CostEstimate(flops=1 << 28, transcendentals=0, bytes_accessed=16 << 20),
    )(spectral.reshape(owned_y, MZ * 2 * CH, CH))
    mixed = pl.pallas_call(
        mix_kernel,
        out_shape=jax.ShapeDtypeStruct((2 * count, LANES), F32),
        in_specs=[VMEM] * 3,
        out_specs=VMEM,
        compiler_params=pltpu.CompilerParams(vmem_limit_bytes=20 << 20),
    )(modes.reshape(2 * count, LANES), *matrix)
    columns = all_to_all(mixed.reshape(tiles, 2 * pair, LANES))
    previous = lax.ppermute(
        hidden, "gx", [(i, (i + 1) % devices_x) for i in range(devices_x)]
    )
    branch = convolve(previous, hidden, conv_second, False, False)
    lines = apply_matrix(inverse_x, columns.reshape(-1, LANES))
    own = all_to_all(lines.reshape(devices_x, ROWS, LANES))
    other = lax.ppermute(own, "gy", [(0, 1), (1, 0)])
    result = pl.pallas_call(
        functools.partial(end_kernel, devices_y=devices_y),
        out_shape=jax.ShapeDtypeStruct((cells_x * cells_y, width), F32),
        in_specs=[VMEM] * 6,
        out_specs=VMEM,
        scratch_shapes=[pltpu.VMEM((2 * cells_x * cells_y, MZ * CH), F32)],
        compiler_params=small_grant(),
    )(
        own, other, inverse_y, twiddle_out, branch.reshape(cells_x * cells_y, width),
        jnp.tile(bias, GROUP).reshape(1, LANES),
    )
    return result.reshape(cells_x, cells_y, width)


def solution(mesh):
    in_specs = (
        P(("groups", "gx"), "gy", None),
        P("gy", "gx", None, None, None, None),
        P(),
        P(),
        P(),
    )
    out_specs = P(("groups", "gx"), "gy", None)
    return jax.shard_map(block, mesh=mesh, in_specs=in_specs, out_specs=out_specs, check_vma=False)
```

```python
import functools
import math

import jax
import jax.numpy as jnp
import numpy as np
from jax import lax
from jax.experimental import pallas as pl
from jax.experimental.pallas import tpu as pltpu
from jax.sharding import PartitionSpec as P

CH = 32
NZ = 64
MX = 32
MY = 32
MZ = 16

LANES = 128
GROUP = LANES // CH
ZQ = NZ // GROUP
ROWS = 8
F32 = jnp.float32
BF16 = jnp.bfloat16
VMEM = pl.BlockSpec(memory_space=pltpu.VMEM)


def small_grant():
    return pltpu.CompilerParams(vmem_limit_bytes=12 << 20)


def split(value):
    high = value.astype(BF16)
    return high, (value - high.astype(F32)).astype(BF16)


def host_split(table):
    table = np.asarray(table, np.float32)
    high = table.astype(jnp.bfloat16)
    low = (table - high.astype(np.float32)).astype(jnp.bfloat16)
    return np.stack([high, low])


def dot(a, b):
    return jnp.dot(a, b, preferred_element_type=F32)


def dot3(table_high, table_low, value):
    high, low = split(value)
    return dot(table_high, high) + (dot(table_low, high) + dot(table_high, low))


def gelu(v):
    return v * (1.0 + lax.erf(v * (1.0 / math.sqrt(2.0)))) * 0.5


def kept(count, length):
    return np.array([j if j < count // 2 else length - count + j for j in range(count)])


def rotation(angle):
    return np.array([[np.cos(angle), -np.sin(angle)], [np.sin(angle), np.cos(angle)]])


def forward_tables(cells_x, cells_y, devices_y):
    extent = cells_y * devices_y
    freq = kept(MY, extent)
    owned = MY // devices_y
    table = np.zeros((devices_y, devices_y, owned, cells_x, 2, 2, cells_x, cells_y))
    for g in range(devices_y):
        places = g * cells_y + np.arange(cells_y)
        for t in range(devices_y):
            rows = freq[t * owned : (t + 1) * owned]
            turn = rotation(-2 * np.pi * (rows[:, None] * places[None, :] % extent) / extent)
            for x in range(cells_x):
                table[g, t, :, x, :, :, x, :] = turn.transpose(2, 0, 1, 3)
    return table.reshape(devices_y, devices_y, owned * cells_x * 2, 2 * cells_x * cells_y)


def z_twiddle(sign):
    zr = np.repeat(np.arange(GROUP), CH)
    angle = sign * 2 * np.pi * np.arange(MZ)[:, None] * zr[None, :] / NZ
    return np.stack([np.cos(angle), np.sin(angle)]).astype(np.float32)


def z_forward(blocks, twiddle, lane):
    half = ZQ // 2
    even = [None] + [blocks[n] + blocks[ZQ - n] for n in range(1, half)]
    odd = [None] + [blocks[n] - blocks[ZQ - n] for n in range(1, half)]
    real, imag = [], []
    for k in range(half + 1):
        re = blocks[0] + blocks[half] if k % 2 == 0 else blocks[0] - blocks[half]
        im = None
        for n in range(1, half):
            c = math.cos(2 * math.pi * (k * n % ZQ) / ZQ)
            s = math.sin(2 * math.pi * (k * n % ZQ) / ZQ)
            if abs(c) > 1e-9:
                re = re + even[n] * c
            if abs(s) > 1e-9:
                im = odd[n] * -s if im is None else im - odd[n] * s
        real.append(re)
        imag.append(im)
    out = ([], [])
    upper = lane >= LANES // 2
    odd_group = (lane // CH) % 2 == 1
    for first in range(0, MZ, GROUP):
        pieces = ([], [])
        for k in range(first, first + GROUP):
            fold = k if k <= half else ZQ - k
            fr, fi = real[fold], imag[fold]
            if fi is not None and k > half:
                fi = -fi
            tc, ts = twiddle(k)
            if fi is None:
                pieces[0].append(fr * tc)
                pieces[1].append(fr * ts)
            else:
                pieces[0].append(fr * tc - fi * ts)
                pieces[1].append(fi * tc + fr * ts)
        for part in range(2):
            y0, y1, y2, y3 = pieces[part]
            a = jnp.where(upper, y2, y0) + pltpu.roll(jnp.where(upper, y0, y2), LANES // 2, 1)
            b = jnp.where(upper, y3, y1) + pltpu.roll(jnp.where(upper, y1, y3), LANES // 2, 1)
            out[part].append(
                jnp.where(odd_group, b + pltpu.roll(b, CH, 1), a + pltpu.roll(a, LANES - CH, 1))
            )
    return out


def forward_kernel(cells_ref, table_ref, keep_ref, send_ref, z_ref, *, devices_y):
    rows = cells_ref.shape[0]
    here = lax.axis_index("gy")
    there = devices_y - 1 - here
    size = keep_ref.shape[0] * ROWS // (MZ // GROUP)
    twiddles = devices_y * devices_y * size
    lane = lax.broadcasted_iota(jnp.int32, (ROWS, LANES), 1)

    def step(i, carry):
        start = pl.multiple_of(i * ROWS, ROWS)
        blocks = [cells_ref[pl.ds(start, ROWS), q * LANES : (q + 1) * LANES] for q in range(ZQ)]

        def twiddle(k):
            return tuple(
                jnp.broadcast_to(table_ref[row : row + 1, :], (ROWS, LANES))
                for row in (twiddles + k, twiddles + MZ + k)
            )

        real, imag = z_forward(blocks, twiddle, lane)
        for h in range(MZ // GROUP):
            z_ref[pl.ds(start, ROWS), h * LANES : (h + 1) * LANES] = real[h]
            z_ref[pl.ds(start + rows, ROWS), h * LANES : (h + 1) * LANES] = imag[h]
        return carry

    lax.fori_loop(0, rows // ROWS, step, 0)
    high, low = split(z_ref[...])
    for target, out_ref in ((there, send_ref), (here, keep_ref)):
        first = pl.multiple_of((here * devices_y + target) * size, size)
        table, table_low = split(table_ref[pl.ds(first, size), :])
        modes = dot(table, high) + (dot(table_low, high) + dot(table, low))
        for h in range(MZ // GROUP):
            for kp in range(modes.shape[0] // ROWS):
                out_ref[h * (modes.shape[0] // ROWS) + kp] = modes[
                    kp * ROWS : (kp + 1) * ROWS, h * LANES : (h + 1) * LANES
                ]


def x_tables(cells_x, devices_x, pair):
    extent = cells_x * devices_x
    freq = kept(MX, extent)
    place = np.arange(extent)
    forward = np.zeros((MX, pair, 2, devices_x, pair, cells_x, 2))
    inverse = np.zeros((devices_x, pair, cells_x, 2, MX, pair, 2))
    angle = 2 * np.pi * (freq[:, None] * place[None, :] % extent) / extent
    turn = rotation(-angle).reshape(2, 2, MX, devices_x, cells_x)
    back = rotation(angle).reshape(2, 2, MX, devices_x, cells_x)
    for q in range(pair):
        forward[:, q, :, :, q] = turn.transpose(2, 0, 3, 4, 1)
        inverse[:, q, :, :, :, q] = back.transpose(3, 4, 0, 2, 1)
    return (
        forward.reshape(MX * pair * 2, devices_x * pair * cells_x * 2),
        inverse.reshape(devices_x * pair * cells_x * 2, MX * pair * 2),
    )


def matrix_kernel(table_ref, value_ref, out_ref):
    out_ref[...] = dot3(table_ref[0], table_ref[1], value_ref[...])


def apply_matrix(table, value):
    return pl.pallas_call(
        matrix_kernel,
        out_shape=jax.ShapeDtypeStruct((table.shape[1], value.shape[1]), F32),
        in_specs=[VMEM, VMEM],
        out_specs=VMEM,
        compiler_params=small_grant(),
    )(table, value)


def prepare_kernel(weight_ref, high_ref, low_ref):
    depth = high_ref.shape[2]

    def step(i, carry):
        for block in range(MZ // GROUP):
            first = block * GROUP * depth
            value = jnp.concatenate(
                [
                    weight_ref[i, first + g * depth : first + (g + 1) * depth, :]
                    for g in range(GROUP)
                ],
                axis=1,
            )
            high_ref[block, i], low_ref[block, i] = split(value)
        return carry

    lax.fori_loop(0, weight_ref.shape[0], step, 0)


def mix_kernel(modes_ref, weight_high_ref, weight_low_ref, out_ref):
    owned_y, depth = weight_high_ref.shape[1:3]
    channels = depth // 2
    span = owned_y * depth
    repeats = span // LANES
    lane = lax.broadcasted_iota(jnp.int32, (owned_y, LANES), 1)
    group = lane // channels
    second = group % 2 == 1
    both_group = lax.broadcasted_iota(jnp.int32, (2 * owned_y, LANES), 1) // channels
    wide_lane = lax.broadcasted_iota(jnp.int32, (2 * owned_y, span), 1)
    wide_row = lax.broadcasted_iota(jnp.int32, (2 * owned_y, span), 0)
    own = wide_lane // depth == wide_row % owned_y

    def spread(value, g):
        value = jnp.where(group == g, value, 0.0)
        value = value + pltpu.roll(value, LANES // 2, 1)
        return value + pltpu.roll(value, channels, 1)

    for block in range(MZ // GROUP):
        first = block * 2 * owned_y
        real = modes_ref[pl.ds(first, owned_y, stride=2), :]
        imag = modes_ref[pl.ds(first + 1, owned_y, stride=2), :]
        left = ([], [])
        for g in range(GROUP):
            re, im = spread(real, g), spread(imag, g)
            pair = jnp.concatenate([jnp.where(second, -im, re), jnp.where(second, re, im)], axis=0)
            for part, value in zip(left, split(pair), strict=True):
                wide = jnp.concatenate([value.astype(F32)] * repeats, axis=1)
                part.append(jnp.where(own, wide, 0.0).astype(BF16))
        high, low = (jnp.concatenate(part, axis=0) for part in left)
        weight_high = weight_high_ref[block].reshape(span, LANES)
        weight_low = weight_low_ref[block].reshape(span, LANES)
        total = dot(high, weight_high) + (dot(low, weight_high) + dot(high, weight_low))
        mixed = total[: 2 * owned_y]
        for g in range(1, GROUP):
            mixed = jnp.where(
                both_group == g, total[g * 2 * owned_y : (g + 1) * 2 * owned_y], mixed
            )
        out_ref[pl.ds(first, owned_y, stride=2), :] = mixed[:owned_y]
        out_ref[pl.ds(first + 1, owned_y, stride=2), :] = mixed[owned_y:]


def inverse_tables(cells_x, cells_y, devices_y):
    extent = cells_y * devices_y
    freq = kept(MY, extent)
    owned = MY // devices_y
    table = np.zeros((devices_y, devices_y, 2, cells_x, cells_y, owned, cells_x, 2))
    for g in range(devices_y):
        places = g * cells_y + np.arange(cells_y)
        for t in range(devices_y):
            rows = freq[t * owned : (t + 1) * owned]
            turn = rotation(2 * np.pi * (places[:, None] * rows[None, :] % extent) / extent)
            for x in range(cells_x):
                table[g, t, :, x, :, :, x, :] = turn.transpose(0, 2, 3, 1)
    return table.reshape(devices_y, devices_y, 2 * cells_x * cells_y, owned * cells_x * 2)


def end_kernel(
    own_ref, other_ref, table_ref, twiddle_ref, branch_ref, bias_ref, out_ref, y_ref, *, devices_y
):
    here = lax.axis_index("gy")
    there = devices_y - 1 - here
    wide = MZ // GROUP
    rows = out_ref.shape[0]

    def gather(ref):
        pairs = ref.shape[0] // wide
        return jnp.concatenate(
            [
                jnp.concatenate([ref[h * pairs + kp] for kp in range(pairs)], axis=0)
                for h in range(wide)
            ],
            axis=1,
        )

    y_ref[...] = dot3(table_ref[here, here, 0], table_ref[here, here, 1], gather(own_ref)) + dot3(
        table_ref[here, there, 0], table_ref[here, there, 1], gather(other_ref)
    )
    lane = lax.broadcasted_iota(jnp.int32, (ROWS, LANES), 1)
    group = lane // CH
    half = ZQ // 2

    def step(i, carry):
        start = pl.multiple_of(i * ROWS, ROWS)

        def spread(value, g):
            kept_lanes = jnp.where(group == g, value, 0.0)
            kept_lanes = kept_lanes + pltpu.roll(kept_lanes, LANES // 2, 1)
            return kept_lanes + pltpu.roll(kept_lanes, CH, 1)

        real, imag = [], []
        for k in range(MZ):
            h, g = divmod(k, GROUP)
            re = spread(y_ref[pl.ds(start, ROWS), h * LANES : (h + 1) * LANES], g)
            im = spread(y_ref[pl.ds(start + rows, ROWS), h * LANES : (h + 1) * LANES], g)
            tc = jnp.broadcast_to(twiddle_ref[0, k : k + 1, :], (ROWS, LANES))
            ts = jnp.broadcast_to(twiddle_ref[1, k : k + 1, :], (ROWS, LANES))
            real.append(re * tc - im * ts)
            imag.append(re * ts + im * tc)
        even = [None] + [real[k] + real[ZQ - k] for k in range(1, half)]
        odd = [None] + [imag[k] - imag[ZQ - k] for k in range(1, half)]
        bias = jnp.broadcast_to(bias_ref[...], (ROWS, LANES))
        for q in range(half + 1):
            cos_part = real[0] + real[half] if q % 2 == 0 else real[0] - real[half]
            cos_part = cos_part + bias
            sin_part = None
            for k in range(1, half):
                c = math.cos(2 * math.pi * (k * q % ZQ) / ZQ)
                s = math.sin(2 * math.pi * (k * q % ZQ) / ZQ)
                if abs(c) > 1e-9:
                    cos_part = cos_part + even[k] * c
                if abs(s) > 1e-9:
                    sin_part = odd[k] * s if sin_part is None else sin_part + odd[k] * s
            places = [(q, -1.0)] if sin_part is None else [(q, -1.0), (ZQ - q, 1.0)]
            for place, sign in places:
                value = cos_part
                if sin_part is not None:
                    value = cos_part + sin_part if sign > 0 else cos_part - sin_part
                lanes = slice(place * LANES, (place + 1) * LANES)
                value = value + branch_ref[pl.ds(start, ROWS), lanes]
                out_ref[pl.ds(start, ROWS), lanes] = gelu(value)
        return carry

    lax.fori_loop(0, rows // ROWS, step, 0)


BLOCK = 8
WINDOW = BLOCK + 2 * GROUP
TOP = 8


def conv_kernel(
    first_ref, second_ref, rim_ref, weight_ref, out_ref, pad_ref, high_ref, low_ref,
    table_high_ref, table_low_ref, acc_ref, *, shifted, activate,
):
    cells_ref = first_ref
    cells_x, cells_y, width = cells_ref.shape
    here = lax.axis_index("gy")
    blocks = NZ // BLOCK
    out_lanes = BLOCK * CH
    in_lanes = WINDOW * CH

    lane = lax.broadcasted_iota(jnp.int32, (CH, out_lanes), 1)
    group = lane // CH
    repeat = jnp.where(
        lax.broadcasted_iota(jnp.int32, (CH, out_lanes), 0) == lane % CH, 1.0, 0.0
    ).astype(BF16)
    zero = jnp.zeros((CH, out_lanes), BF16)

    def build(i, carry):
        for value, ref in zip(split(weight_ref[i]), (table_high_ref, table_low_ref), strict=True):
            wide = dot(value, repeat)
            for z in range(WINDOW):
                total = None
                for e in range(3):
                    place = z - (GROUP - 1) - e
                    if 0 <= place < BLOCK:
                        other = 0.0 if total is None else total
                        total = jnp.where(group == place, wide[e * CH : (e + 1) * CH], other)
                ref[i, z * CH : (z + 1) * CH, :] = zero if total is None else total.astype(BF16)
        return carry

    lax.fori_loop(0, 9, build, 0)

    pad_ref[:, :, :LANES] = jnp.zeros((2 * cells_x, pad_ref.shape[1], LANES), F32)
    pad_ref[:, :, LANES + width :] = jnp.zeros((2 * cells_x, pad_ref.shape[1], LANES), F32)
    inner = slice(LANES, LANES + width)
    for x in range(cells_x):
        pad_ref[x, TOP : TOP + cells_y, inner] = first_ref[x]
        pad_ref[cells_x + x, TOP : TOP + cells_y, inner] = second_ref[x]
    for x in range(2 * cells_x):
        row = rim_ref[x : x + 1, :]
        pad_ref[x, TOP - 1 : TOP, inner] = jnp.where(here == 0, 0.0, row)
        pad_ref[x, TOP + cells_y : TOP + cells_y + 1, inner] = jnp.where(here == 0, row, 0.0)

    place = lax.axis_index("gx")
    at_start = place == 0
    at_end = place == lax.axis_size("gx") - 1

    def fill(slot, carry):
        x = (slot + 1) // 2
        if shifted:
            outside = at_end & ((slot == 1) | (slot == 4))
        else:
            outside = (at_start & (slot == 0)) | (at_end & (slot == 5))
        inside = jnp.where(outside, 0.0, 1.0)
        for shift in range(3):
            for z in range(pad_ref.shape[2] // out_lanes):
                lanes = slice(z * out_lanes, (z + 1) * out_lanes)
                value = pad_ref[x, TOP - 1 + shift : TOP - 1 + shift + cells_y, lanes]
                high, low = split(value * inside)
                high_ref[shift, slot, :, lanes] = high
                low_ref[shift, slot, :, lanes] = low
        return carry

    lax.fori_loop(0, 3 * cells_x, fill, 0)

    acc_ref[...] = jnp.zeros(acc_ref.shape, F32)

    def multiply(i, carry):
        shift_x = i // 3
        shift_y = i % 3
        high, low = (
            jnp.concatenate(
                [
                    ref[
                        shift_y,
                        pl.ds(shift_x * cells_x, cells_x),
                        :,
                        z * out_lanes : z * out_lanes + in_lanes,
                    ].reshape(cells_x * cells_y, in_lanes)
                    for z in range(blocks)
                ],
                axis=0,
            )
            for ref in (high_ref, low_ref)
        )
        table_high = table_high_ref[i]
        acc_ref[...] += dot(high, table_high) + (
            dot(high, table_low_ref[i]) + dot(low, table_high)
        )
        return carry

    lax.fori_loop(0, 9, multiply, 0)
    for z in range(blocks):
        for x in range(cells_x):
            start = (z * cells_x + x) * cells_y
            value = acc_ref[start : start + cells_y, :]
            out_ref[x, :, z * out_lanes : (z + 1) * out_lanes] = gelu(value) if activate else value


def rim_kernel(first_top, first_end, second_top, second_end, out_ref):
    here = lax.axis_index("gy")
    for i, (top, end) in enumerate(((first_top, first_end), (second_top, second_end))):
        for x in range(top.shape[0]):
            row = jnp.where(here == 0, end[x, ROWS - 1 : ROWS, :], top[x, 0:1, :])
            out_ref[i * top.shape[0] + x : i * top.shape[0] + x + 1, :] = row


def convolve(first, second, weight, shifted, activate):
    cells_x, cells_y, width = first.shape
    top = pl.BlockSpec((cells_x, ROWS, width), lambda i: (0, 0, 0))
    end = pl.BlockSpec((cells_x, ROWS, width), lambda i: (0, cells_y // ROWS - 1, 0))
    rim = pl.pallas_call(
        rim_kernel,
        grid=(1,),
        out_shape=jax.ShapeDtypeStruct((2 * cells_x, width), F32),
        in_specs=[top, end, top, end],
        out_specs=pl.BlockSpec((2 * cells_x, width), lambda i: (0, 0)),
        compiler_params=small_grant(),
    )(first, first, second, second)
    rim = lax.ppermute(rim, "gy", [(0, 1), (1, 0)])
    return band_product(first, second, rim, weight, shifted, activate)


def band_product(first, second, rim, weight, shifted, activate):
    cells_x, cells_y, width = first.shape
    blocks = NZ // BLOCK
    rows = blocks * cells_x * cells_y
    return pl.pallas_call(
        functools.partial(conv_kernel, shifted=shifted, activate=activate),
        out_shape=jax.ShapeDtypeStruct(first.shape, F32),
        in_specs=[VMEM] * 4,
        out_specs=VMEM,
        scratch_shapes=[
            pltpu.VMEM((2 * cells_x, cells_y + 2 * TOP, width + 2 * LANES), F32),
            pltpu.VMEM((3, 3 * cells_x, cells_y, width + 2 * LANES), BF16),
            pltpu.VMEM((3, 3 * cells_x, cells_y, width + 2 * LANES), BF16),
            pltpu.VMEM((9, WINDOW * CH, BLOCK * CH), BF16),
            pltpu.VMEM((9, WINDOW * CH, BLOCK * CH), BF16),
            pltpu.VMEM((rows, BLOCK * CH), F32),
        ],
        compiler_params=pltpu.CompilerParams(vmem_limit_bytes=20 << 20),
        cost_estimate=pl.CostEstimate(
            flops=6 * rows * 9 * WINDOW * CH * BLOCK * CH, transcendentals=0, bytes_accessed=1 << 21
        ),
    )(first, second, rim, weight.reshape(9, 3 * CH, CH))


def all_to_all(value):
    return lax.all_to_all(value, "gx", split_axis=0, concat_axis=0, tiled=True)


def block(field, spectral, conv_first, conv_second, bias):
    cells_x, cells_y, width = field.shape
    devices_x = lax.axis_size("gx")
    devices_y = lax.axis_size("gy")
    extent_x = cells_x * devices_x
    extent_y = cells_y * devices_y
    owned_y = MY // devices_y
    wide = MZ // GROUP
    pair = ROWS // (2 * cells_x)
    tiles = owned_y // pair * wide
    assert devices_y == 2 and cells_x == 2 and tiles == devices_x and MX == devices_x

    forward_y = np.concatenate(
        [
            forward_tables(cells_x, cells_y, devices_y).reshape(-1, 2 * cells_x * cells_y),
            z_twiddle(-1).reshape(-1, LANES),
        ]
    ).astype(np.float32)
    inverse_y = np.moveaxis(host_split(inverse_tables(cells_x, cells_y, devices_y)), 0, 2)
    forward_x, inverse_x = (host_split(t) for t in x_tables(cells_x, devices_x, pair))
    twiddle_out = z_twiddle(1)
    weights = np.where(np.arange(MZ) == 0, 1.0, 2.0) / (extent_x * extent_y * NZ)
    twiddle_out = (twiddle_out * weights[None, :, None]).astype(np.float32)

    tile_shape = jax.ShapeDtypeStruct((tiles, ROWS, LANES), F32)
    keep, send = pl.pallas_call(
        functools.partial(forward_kernel, devices_y=devices_y),
        out_shape=(tile_shape, tile_shape),
        in_specs=[VMEM] * 2,
        out_specs=(VMEM, VMEM),
        scratch_shapes=[pltpu.VMEM((2 * cells_x * cells_y, MZ * CH), F32)],
        compiler_params=small_grant(),
    )(field.reshape(cells_x * cells_y, width), forward_y)
    lines = keep + lax.ppermute(send, "gy", [(0, 1), (1, 0)])
    lines, cells = lax.optimization_barrier((lines, field))

    columns = all_to_all(lines)
    following = lax.ppermute(
        cells, "gx", [((i + 1) % devices_x, i) for i in range(devices_x)]
    )
    hidden = convolve(cells, following, conv_first, True, True)
    modes = apply_matrix(forward_x, columns.reshape(-1, LANES))
    modes = all_to_all(modes.reshape(MX, 2 * pair, LANES))

    count = tiles * pair
    matrix_shape = (wide, owned_y, 2 * CH, LANES)
    matrix = pl.pallas_call(
        prepare_kernel,
        out_shape=(jax.ShapeDtypeStruct(matrix_shape, BF16),) * 2,
        in_specs=[VMEM],
        out_specs=(VMEM, VMEM),
        compiler_params=pltpu.CompilerParams(vmem_limit_bytes=20 << 20),
        cost_estimate=pl.CostEstimate(flops=1 << 28, transcendentals=0, bytes_accessed=16 << 20),
    )(spectral.reshape(owned_y, MZ * 2 * CH, CH))
    mixed = pl.pallas_call(
        mix_kernel,
        out_shape=jax.ShapeDtypeStruct((2 * count, LANES), F32),
        in_specs=[VMEM] * 3,
        out_specs=VMEM,
        compiler_params=pltpu.CompilerParams(vmem_limit_bytes=20 << 20),
    )(modes.reshape(2 * count, LANES), *matrix)
    columns = all_to_all(mixed.reshape(tiles, 2 * pair, LANES))
    previous = lax.ppermute(
        hidden, "gx", [(i, (i + 1) % devices_x) for i in range(devices_x)]
    )
    branch = convolve(previous, hidden, conv_second, False, False)
    lines = apply_matrix(inverse_x, columns.reshape(-1, LANES))
    own = all_to_all(lines.reshape(devices_x, ROWS, LANES))
    other = lax.ppermute(own, "gy", [(0, 1), (1, 0)])
    result = pl.pallas_call(
        functools.partial(end_kernel, devices_y=devices_y),
        out_shape=jax.ShapeDtypeStruct((cells_x * cells_y, width), F32),
        in_specs=[VMEM] * 6,
        out_specs=VMEM,
        scratch_shapes=[pltpu.VMEM((2 * cells_x * cells_y, MZ * CH), F32)],
        compiler_params=small_grant(),
    )(
        own, other, inverse_y, twiddle_out, branch.reshape(cells_x * cells_y, width),
        jnp.tile(bias, GROUP).reshape(1, LANES),
    )
    return result.reshape(cells_x, cells_y, width)


def solution(mesh):
    in_specs = (
        P(("groups", "gx"), "gy", None),
        P("gy", "gx", None, None, None, None),
        P(),
        P(),
        P(),
    )
    out_specs = P(("groups", "gx"), "gy", None)
    return jax.shard_map(block, mesh=mesh, in_specs=in_specs, out_specs=out_specs, check_vma=False)
```
